256 devices in a mesh: ep: 64 (over z, y, core), fsdp: 4 (over x).
Axes of the slice: x: 4, y: 4, z: 8, core: 2. Of those that a mesh axis runs over, the one named last changes fastest.
Arguments:
- w_down: float32 [64, 1408, 2048], P('ep', None, 'fsdp'), may hold values from -0.21875 to 0.21875
- avg_down: float32 [64, 1408, 2048], P('ep', None, 'fsdp'), may hold values from -0.15625 to 0.15625
- router_weight: float32 [2048, 64], P('fsdp', 'ep'), may hold values from -0.125 to 0.125
- router_gain: float32 [2048], P('fsdp'), may hold values from 0.25 to 1.75
Outputs:
- serve_down: bfloat16 [64, 1408, 2048], P('ep')
- scale_down: float32 [64, 1408], P('ep')
- serve_router: bfloat16 [2048, 64], replicated
- fresh_down: float32 [64, 1408, 2048], P('ep', None, 'fsdp')
The draws below stay inside these ranges and needn't reach their ends.
All inputs are finite; a program needn't handle non-finite values. Where the reference program divides by a largest or mean magnitude, that divisor is 1e-20 or more.
Results may differ from the reference program's by a relative error of at most 0.001.
Values may be sent and summed in bfloat16 or wider, within the bound.
A program may use at most 64 MiB of HBM per device.

```python
import jax
import jax.numpy as jnp

EXPERTS = 64
D_MODEL = 2048
D_EXPERT = 1408


def raised(array, key, source, target, parts, factor):
    owner, partner = [(jnp.arange(array.shape[position]) // (array.shape[position] // parts)).reshape([-1 if axis == position else 1 for axis in range(array.ndim)]) for position in (source, target)]
    chosen = jax.random.permutation(key, parts)[partner]
    strong = (owner == chosen) | (owner == (partner + parts // 2) % parts)
    return jnp.where(strong, factor * array, array)


def shard_levels(stream_key, extent, split, low, largest):
    gain = 1.0
    for axis_at, parts in split:
        steps = jax.random.uniform(jax.random.fold_in(jax.random.fold_in(stream_key, 6), axis_at), (parts,), jnp.float32, low / len(split), largest / len(split))
        gain = gain * jnp.repeat(jnp.exp(steps), extent[axis_at] // parts).reshape((-1,) + (1,) * (len(extent) - 1 - axis_at))
    return gain


def normal_values(own_key, shape, scale, reach, split=(), dtype=jnp.bfloat16):
    loudness = shard_levels(own_key, shape, split, -0.22, 0.18) if split else 1.0
    drawn = jax.random.normal(own_key, shape, jnp.float32) * scale * loudness
    return jnp.minimum(jnp.maximum(drawn, -reach), reach).astype(dtype)


def heavy_noise(rng, shape, scale, limit, cuts, heavy, held_as=jnp.bfloat16):
    drawn = scale * jax.random.normal(rng, shape, jnp.float32)
    if cuts:
        drawn = drawn * shard_levels(rng, shape, cuts, -0.22, 0.18)
    return jnp.clip(raised(drawn, jax.random.fold_in(rng, 3), *heavy), -limit, limit).astype(held_as)


def setup_inputs(seed: int = 0) -> dict:
    splits = jax.random.split(jax.random.key(seed), 5)
    w_down = heavy_noise(splits[0], (EXPERTS, D_EXPERT, D_MODEL), D_EXPERT ** -0.5, 0.21875, ((0, 64), (2, 4)), (2, 1, 4, 2.0), jnp.float32)
    avg_down = normal_values(splits[1], (EXPERTS, D_EXPERT, D_MODEL), D_EXPERT ** -0.5, 0.15625, ((0, 64), (2, 4)), jnp.float32)
    router_weight = normal_values(splits[2], (D_MODEL, EXPERTS), D_MODEL ** -0.5, 0.125, ((0, 4), (1, 64)), jnp.float32)
    router_gain = jnp.clip(1.0 + 0.15 * jax.random.normal(splits[3], (D_MODEL,), jnp.float32), 0.25, 1.75)
    return {"w_down": w_down, "avg_down": avg_down, "router_weight": router_weight, "router_gain": router_gain}


def reference(w_down, avg_down, router_weight, router_gain):
    fresh_down = 0.5 * avg_down + 0.5 * w_down
    scale_down = jnp.max(jnp.abs(fresh_down), axis=2)
    serve_down = (fresh_down / jnp.expand_dims(scale_down, 2)).astype(jnp.bfloat16)
    serve_router = (router_weight * router_gain[:, None]).astype(jnp.bfloat16)
    return serve_down, scale_down, serve_router, fresh_down
```

```python
import jax
import jax.numpy as jnp
from jax import lax
from jax.experimental import pallas as pl
from jax.experimental.pallas import tpu as pltpu
from jax.sharding import PartitionSpec as P

MESH = pl.DeviceIdType.MESH
F32, BF16 = jnp.float32, jnp.bfloat16
NX, NY, NZ, NC = 4, 4, 8, 2
ROWS, COLS = 1408, 512
WIDE = NX * COLS
HALF = COLS // 2
BLK = 128
NB = ROWS // BLK


def rows_of(b):
    return pl.ds(pl.multiple_of(b * BLK, BLK), BLK)


def gather_kernel(
    w_hbm, a_hbm, rw_hbm, gain_hbm, serve, fresh, scale, router,
    wbuf, abuf, rw, gain, m0, m1, piece, wide,
    load_sem, small_sem, m_send, m_recv, own_send, own_recv, fwd_send, fwd_recv,
    r0_send, r0_recv, r1_send, r1_recv, r2_send, r2_recv, r3_send, r3_recv,
):
    x, e = lax.axis_index("fsdp"), lax.axis_index("ep")
    right, far, left = lax.rem(x + 1, NX), lax.rem(x + 2, NX), lax.rem(x + 3, NX)
    lo = lax.rem(e, NY * NC)
    z, y, c = e // (NY * NC), lo // NC, lax.rem(lo, NC)
    x_peers = ({"fsdp": right}, {"fsdp": left}, {"fsdp": far})
    mate = {"ep": e + 1 - 2 * c}
    y_up = {"ep": z * (NY * NC) + lax.rem(y + 1, NY) * NC + c}
    y_down = {"ep": z * (NY * NC) + lax.rem(y + NY - 1, NY) * NC + c}
    z_up = {"ep": lax.rem(z + 1, NZ) * (NY * NC) + lo}
    z_down = {"ep": lax.rem(z + NZ - 1, NZ) * (NY * NC) + lo}

    def load(b, k):
        src, dst = ((w_hbm, wbuf), (a_hbm, abuf))[k]
        return pltpu.make_async_copy(src.at[rows_of(b)], dst.at[rows_of(b)], load_sem.at[k, b])

    def start_load(b, carry):
        load(b, 0).start()
        load(b, 1).start()
        return carry

    def remote(src, dst, send, recv, peer):
        return pltpu.make_async_remote_copy(
            src_ref=src, dst_ref=dst, send_sem=send, recv_sem=recv, device_id=peer, device_id_type=MESH
        )

    small = [
        pltpu.make_async_copy(rw_hbm, rw, small_sem.at[0]),
        pltpu.make_async_copy(gain_hbm, gain, small_sem.at[1]),
    ]
    start_load(0, 0)
    for copy in small:
        copy.start()
    lax.fori_loop(1, NB, start_load, 0)

    barrier = pltpu.get_barrier_semaphore()
    peers = (*x_peers, mate, y_up, y_down, z_up, z_down)
    for peer in peers:
        pl.semaphore_signal(barrier, inc=1, device_id=peer, device_id_type=MESH)

    def average(b):
        load(b, 0).wait()
        load(b, 1).wait()
        here = rows_of(b)
        top = None
        for k in range(COLS // 128):
            lanes = pl.ds(k * 128, 128)
            value = 0.5 * abuf[here, lanes] + 0.5 * wbuf[here, lanes]
            fresh[here, lanes] = value
            top = jnp.abs(value) if top is None else jnp.maximum(top, jnp.abs(value))
        return jnp.max(top.T, axis=0, keepdims=True)

    m0[x] = average(0)
    for copy in small:
        copy.wait()
    part = rw[...] * gain[...]
    for k in range(NX):
        piece[lo, x, k : k + 1, :] = part[:, k * 128 : (k + 1) * 128]
    pl.semaphore_wait(barrier, len(peers))

    first = [remote(m0.at[x], m0.at[x], m_send.at[0, k], m_recv.at[0, k], x_peers[k]) for k in range(3)]
    rest = [remote(m1.at[x], m1.at[x], m_send.at[1, k], m_recv.at[1, k], x_peers[k]) for k in range(3)]
    r0 = [remote(piece.at[lo, x], piece.at[lo, x], r0_send.at[k], r0_recv.at[k], x_peers[k]) for k in range(3)]
    for copy in first:
        copy.start()
    for copy in r0:
        copy.start()

    def maxima(b, carry):
        m1[x, pl.ds(b - 1, 1), :] = average(b)
        return carry

    lax.fori_loop(1, NB, maxima, 0)
    for copy in rest:
        copy.start()

    mine = x * COLS

    def own(b, h, d):
        ref = serve.at[rows_of(b), pl.ds(pl.multiple_of(mine + h * HALF, HALF), HALF)]
        return remote(ref, ref, own_send.at[d, h, b], own_recv.at[d, h, b], x_peers[d])

    def forward(b, d):
        start = (left if d == 0 else right) * COLS + d * HALF
        ref = serve.at[rows_of(b), pl.ds(pl.multiple_of(start, HALF), HALF)]
        return remote(ref, ref, fwd_send.at[d, b], fwd_recv.at[d, b], x_peers[d])

    def narrow(b, top):
        here = rows_of(b)
        scale[:, pl.ds(pl.multiple_of(b * BLK, BLK), BLK)] = top
        tall = jnp.broadcast_to(top, (BLK, BLK)).T
        for k in range(COLS // 128):
            value = fresh[here, pl.ds(k * 128, 128)] / tall
            serve[here, pl.ds(pl.multiple_of(mine + k * 128, 128), 128)] = value.astype(BF16)

    for copy in first:
        copy.wait_recv()
    narrow(0, jnp.maximum(jnp.maximum(m0[0], m0[1]), jnp.maximum(m0[2], m0[3])))
    own(0, 0, 0).start()
    own(0, 1, 1).start()
    own(0, 1, 0).start()
    own(0, 0, 1).start()
    for copy in rest:
        copy.wait_recv()

    def first_halves(b, carry):
        at = pl.ds(b - 1, 1)
        narrow(b, jnp.maximum(jnp.maximum(m1[0, at], m1[1, at]), jnp.maximum(m1[2, at], m1[3, at])))
        own(b, 0, 0).start()
        own(b, 1, 1).start()
        return carry

    def second_halves(b, carry):
        own(b, 1, 0).start()
        own(b, 0, 1).start()
        return carry

    lax.fori_loop(1, NB, first_halves, 0)
    lax.fori_loop(1, NB, second_halves, 0)

    for copy in r0:
        copy.wait_recv()
    r1 = remote(piece.at[lo], piece.at[lo], r1_send, r1_recv, mate)
    r1.start()
    r1.wait_recv()
    chip = piece.at[pl.ds(y * NC, NC)]
    below = piece.at[pl.ds(lax.rem(y + NY - 1, NY) * NC, NC)]
    r2 = [
        remote(chip, chip, r2_send.at[0], r2_recv.at[0], y_up),
        remote(chip, chip, r2_send.at[1], r2_recv.at[1], y_down),
        remote(below, below, r2_send.at[2], r2_recv.at[2], y_up),
    ]
    r2[0].start()
    r2[1].start()
    r2[0].wait_recv()
    r2[2].start()
    r2[1].wait_recv()
    r2[2].wait_recv()
    for i in range(NY * NC):
        for k in range(WIDE // 128):
            wide[i : i + 1, k * 128 : (k + 1) * 128] = piece[i, k // 4, k % 4 : k % 4 + 1, :]
    router[z] = wide[...].astype(BF16)
    r3 = []
    for k in range(NZ // 2):
        for d, peer in ((0, z_up), (1, z_down)):
            if d == 1 and k == NZ // 2 - 1:
                continue
            plane = router.at[lax.rem(z + (NZ - k if d == 0 else k), NZ)]
            r3.append((k, d, remote(plane, plane, r3_send.at[d, k], r3_recv.at[d, k], peer)))
    for k in range(NZ // 2):
        for step, d, copy in r3:
            if step == k:
                copy.start()
        for step, d, copy in r3:
            if step == k:
                copy.wait_recv()

    def pass_on(b, carry):
        own(b, 0, 0).wait_recv()
        forward(b, 0).start()
        own(b, 1, 1).wait_recv()
        forward(b, 1).start()
        return carry

    lax.fori_loop(0, NB, pass_on, 0)

    def finish(b, carry):
        own(b, 1, 0).wait_recv()
        own(b, 0, 1).wait_recv()
        for d in range(2):
            forward(b, d).wait_recv()
            for h in range(2):
                own(b, h, d).wait_send()
            forward(b, d).wait_send()
        return carry

    lax.fori_loop(0, NB, finish, 0)
    for copy in (*first, *rest, *r0, r1, *r2, *[step[2] for step in r3]):
        copy.wait_send()


def gather(w_down, avg_down, rw, gain):
    dma, any_, vmem = pltpu.SemaphoreType.DMA, pl.BlockSpec(memory_space=pl.ANY), pl.BlockSpec(memory_space=pltpu.VMEM)
    return pl.pallas_call(
        gather_kernel,
        out_shape=(
            pltpu.VMEM((ROWS, WIDE), BF16),
            pltpu.VMEM((ROWS, COLS), F32),
            pltpu.VMEM((1, ROWS), F32),
            pltpu.VMEM((NZ, NY * NC, WIDE), BF16),
        ),
        in_specs=[any_] * 4,
        out_specs=(vmem, vmem, vmem, vmem),
        scratch_shapes=[
            pltpu.VMEM((ROWS, COLS), F32),
            pltpu.VMEM((ROWS, COLS), F32),
            pltpu.VMEM((1, COLS), F32),
            pltpu.VMEM((1, COLS), F32),
            pltpu.VMEM((NX, 1, BLK), F32),
            pltpu.VMEM((NX, NB - 1, BLK), F32),
            pltpu.VMEM((NY * NC, NX, NX, 128), F32),
            pltpu.VMEM((NY * NC, WIDE), F32),
            dma((2, NB)),
            dma((2,)),
            dma((2, 3)),
            dma((2, 3)),
            dma((2, 2, NB)),
            dma((2, 2, NB)),
            dma((2, NB)),
            dma((2, NB)),
            dma((3,)),
            dma((3,)),
            dma,
            dma,
            dma((3,)),
            dma((3,)),
            dma((2, NZ // 2)),
            dma((2, NZ // 2)),
        ],
        compiler_params=pltpu.CompilerParams(
            collective_id=0, has_side_effects=True, vmem_limit_bytes=24 << 20
        ),
        name="gather",
    )(*(pltpu.with_memory_space_constraint(v, pltpu.HBM) for v in (w_down, avg_down, rw, gain)))


PIECES = 8


def store_kernel(serve, fresh, scale, router, serve_out, fresh_out, scale_out, router_out, sem):
    copies = [
        pltpu.make_async_copy(scale, scale_out, sem.at[0]),
        pltpu.make_async_copy(router, router_out, sem.at[1]),
    ]
    n = ROWS // PIECES
    for k in range(PIECES):
        rows = pl.ds(k * n, n)
        copies.append(pltpu.make_async_copy(serve.at[rows], serve_out.at[rows], sem.at[2 + 2 * k]))
        copies.append(pltpu.make_async_copy(fresh.at[rows], fresh_out.at[rows], sem.at[3 + 2 * k]))
    for copy in copies:
        copy.start()
    for copy in copies:
        copy.wait()


def store(serve, fresh, scale, router):
    vmem, any_ = pl.BlockSpec(memory_space=pltpu.VMEM), pl.BlockSpec(memory_space=pl.ANY)
    return pl.pallas_call(
        store_kernel,
        out_shape=tuple(pltpu.HBM(v.shape, v.dtype) for v in (serve, fresh, scale, router)),
        in_specs=[vmem] * 4,
        out_specs=(any_,) * 4,
        scratch_shapes=[pltpu.SemaphoreType.DMA((2 + 2 * PIECES,))],
        compiler_params=pltpu.CompilerParams(vmem_limit_bytes=16 << 20),
        name="store",
    )(*(pltpu.with_memory_space_constraint(v, pltpu.VMEM) for v in (serve, fresh, scale, router)))


def body(w_down, avg_down, router_weight, router_gain):
    serve, fresh, scale, router = store(
        *gather(
            w_down.reshape(ROWS, COLS),
            avg_down.reshape(ROWS, COLS),
            router_weight.reshape(1, COLS),
            router_gain.reshape(1, COLS),
        )
    )
    return (
        serve.reshape(1, ROWS, WIDE),
        scale,
        router.reshape(NZ * NY * NC, WIDE).T,
        fresh.reshape(1, ROWS, COLS),
    )


def solution(mesh):
    placed = (P("ep", None, "fsdp"), P("ep", None, "fsdp"), P("fsdp", "ep"), P("fsdp"))
    return jax.shard_map(
        body,
        mesh=mesh,
        in_specs=placed,
        out_specs=(P("ep", None, None), P("ep", None), P(), P("ep", None, "fsdp")),
        check_vma=False,
    )
```

```python
import jax
import jax.numpy as jnp
from jax import lax
from jax.experimental import pallas as pl
from jax.experimental.pallas import tpu as pltpu
from jax.sharding import PartitionSpec as P

MESH = pl.DeviceIdType.MESH
F32, BF16 = jnp.float32, jnp.bfloat16
NX, NY, NZ, NC = 4, 4, 8, 2
ROWS, COLS = 1408, 512
WIDE = NX * COLS
HALF = COLS // 2
BLK = 128
NB = ROWS // BLK


def rows_of(b):
    return pl.ds(pl.multiple_of(b * BLK, BLK), BLK)


def gather_kernel(
    w_hbm, a_hbm, rw_hbm, gain_hbm, serve, fresh, scale, router,
    wbuf, abuf, rw, gain, m0, m1, piece, wide,
    load_sem, small_sem, m_send, m_recv, own_send, own_recv, fwd_send, fwd_recv,
    r0_send, r0_recv, r1_send, r1_recv, r2_send, r2_recv, r3_send, r3_recv, greeted,
):
    x, e = lax.axis_index("fsdp"), lax.axis_index("ep")
    right, far, left = lax.rem(x + 1, NX), lax.rem(x + 2, NX), lax.rem(x + 3, NX)
    lo = lax.rem(e, NY * NC)
    z, y, c = e // (NY * NC), lo // NC, lax.rem(lo, NC)
    x_peers = ({"fsdp": right}, {"fsdp": left}, {"fsdp": far})
    mate = {"ep": e + 1 - 2 * c}
    y_up = {"ep": z * (NY * NC) + lax.rem(y + 1, NY) * NC + c}
    y_down = {"ep": z * (NY * NC) + lax.rem(y + NY - 1, NY) * NC + c}
    z_up = {"ep": lax.rem(z + 1, NZ) * (NY * NC) + lo}
    z_down = {"ep": lax.rem(z + NZ - 1, NZ) * (NY * NC) + lo}

    def load(b, k):
        src, dst = ((w_hbm, wbuf), (a_hbm, abuf))[k]
        return pltpu.make_async_copy(src.at[rows_of(b)], dst.at[rows_of(b)], load_sem.at[k, b])

    def start_load(b, carry):
        load(b, 0).start()
        load(b, 1).start()
        return carry

    def remote(src, dst, send, recv, peer):
        return pltpu.make_async_remote_copy(
            src_ref=src, dst_ref=dst, send_sem=send, recv_sem=recv, device_id=peer, device_id_type=MESH
        )

    small = [
        pltpu.make_async_copy(rw_hbm, rw, small_sem.at[0]),
        pltpu.make_async_copy(gain_hbm, gain, small_sem.at[1]),
    ]
    start_load(0, 0)
    for copy in small:
        copy.start()
    lax.fori_loop(1, NB, start_load, 0)

    barrier = pltpu.get_barrier_semaphore()
    for peer in x_peers:
        pl.semaphore_signal(barrier, inc=1, device_id=peer, device_id_type=MESH)
    links = (
        (c == 0, c == 1, mate),
        (y < NY - 1, y == NY - 1, y_up),
        (y == 0, y > 0, y_down),
        (z < NZ - 1, z == NZ - 1, z_up),
        (z == 0, z > 0, z_down),
    )
    entries, greetings = 3, 0
    for leads, follows, peer in links:
        entries += follows.astype(jnp.int32)
        greetings += leads.astype(jnp.int32)

        @pl.when(leads)
        def _(peer=peer):
            pl.semaphore_signal(barrier, inc=1, device_id=peer, device_id_type=MESH)

    def average(b):
        load(b, 0).wait()
        load(b, 1).wait()
        here = rows_of(b)
        top = None
        for k in range(COLS // 128):
            lanes = pl.ds(k * 128, 128)
            value = 0.5 * abuf[here, lanes] + 0.5 * wbuf[here, lanes]
            fresh[here, lanes] = value
            top = jnp.abs(value) if top is None else jnp.maximum(top, jnp.abs(value))
        return jnp.max(top.T, axis=0, keepdims=True)

    m0[x] = average(0)
    for copy in small:
        copy.wait()
    part = rw[...] * gain[...]
    for k in range(NX):
        piece[lo, x, k : k + 1, :] = part[:, k * 128 : (k + 1) * 128]
    pl.semaphore_wait(barrier, entries)
    for _, follows, peer in links:

        @pl.when(follows)
        def _(peer=peer):
            pl.semaphore_signal(greeted, inc=1, device_id=peer, device_id_type=MESH)


    first = [remote(m0.at[x], m0.at[x], m_send.at[0, k], m_recv.at[0, k], x_peers[k]) for k in range(3)]
    rest = [remote(m1.at[x], m1.at[x], m_send.at[1, k], m_recv.at[1, k], x_peers[k]) for k in range(3)]
    r0 = [remote(piece.at[lo, x], piece.at[lo, x], r0_send.at[k], r0_recv.at[k], x_peers[k]) for k in range(3)]
    for copy in first:
        copy.start()
    for copy in r0:
        copy.start()

    def maxima(b, carry):
        m1[x, pl.ds(b - 1, 1), :] = average(b)
        return carry

    lax.fori_loop(1, NB, maxima, 0)
    for copy in rest:
        copy.start()

    mine = x * COLS

    def own(b, h, d):
        ref = serve.at[rows_of(b), pl.ds(pl.multiple_of(mine + h * HALF, HALF), HALF)]
        return remote(ref, ref, own_send.at[d, h, b], own_recv.at[d, h, b], x_peers[d])

    def forward(b, d):
        start = (left if d == 0 else right) * COLS + d * HALF
        ref = serve.at[rows_of(b), pl.ds(pl.multiple_of(start, HALF), HALF)]
        return remote(ref, ref, fwd_send.at[d, b], fwd_recv.at[d, b], x_peers[d])

    def narrow(b, top):
        here = rows_of(b)
        scale[:, pl.ds(pl.multiple_of(b * BLK, BLK), BLK)] = top
        tall = jnp.broadcast_to(top, (BLK, BLK)).T
        for k in range(COLS // 128):
            value = fresh[here, pl.ds(k * 128, 128)] / tall
            serve[here, pl.ds(pl.multiple_of(mine + k * 128, 128), 128)] = value.astype(BF16)

    for copy in first:
        copy.wait_recv()
    narrow(0, jnp.maximum(jnp.maximum(m0[0], m0[1]), jnp.maximum(m0[2], m0[3])))
    own(0, 0, 0).start()
    own(0, 1, 1).start()
    own(0, 1, 0).start()
    own(0, 0, 1).start()
    for copy in rest:
        copy.wait_recv()

    def first_halves(b, carry):
        at = pl.ds(b - 1, 1)
        narrow(b, jnp.maximum(jnp.maximum(m1[0, at], m1[1, at]), jnp.maximum(m1[2, at], m1[3, at])))
        own(b, 0, 0).start()
        own(b, 1, 1).start()
        return carry

    def second_halves(b, carry):
        own(b, 1, 0).start()
        own(b, 0, 1).start()
        return carry

    lax.fori_loop(1, NB, first_halves, 0)
    lax.fori_loop(1, NB, second_halves, 0)

    @pl.when(greetings > 0)
    def _():
        pl.semaphore_wait(greeted, greetings)

    for copy in r0:
        copy.wait_recv()
    r1 = remote(piece.at[lo], piece.at[lo], r1_send, r1_recv, mate)
    r1.start()
    r1.wait_recv()
    chip = piece.at[pl.ds(y * NC, NC)]
    below = piece.at[pl.ds(lax.rem(y + NY - 1, NY) * NC, NC)]
    r2 = [
        remote(chip, chip, r2_send.at[0], r2_recv.at[0], y_up),
        remote(chip, chip, r2_send.at[1], r2_recv.at[1], y_down),
        remote(below, below, r2_send.at[2], r2_recv.at[2], y_up),
    ]
    r2[0].start()
    r2[1].start()
    r2[0].wait_recv()
    r2[2].start()
    r2[1].wait_recv()
    r2[2].wait_recv()
    for i in range(NY * NC):
        for k in range(WIDE // 128):
            wide[i : i + 1, k * 128 : (k + 1) * 128] = piece[i, k // 4, k % 4 : k % 4 + 1, :]
    router[z] = wide[...].astype(BF16)
    r3 = []
    for k in range(NZ // 2):
        for d, peer in ((0, z_up), (1, z_down)):
            if d == 1 and k == NZ // 2 - 1:
                continue
            plane = router.at[lax.rem(z + (NZ - k if d == 0 else k), NZ)]
            r3.append((k, d, remote(plane, plane, r3_send.at[d, k], r3_recv.at[d, k], peer)))
    for k in range(NZ // 2):
        for step, d, copy in r3:
            if step == k:
                copy.start()
        for step, d, copy in r3:
            if step == k:
                copy.wait_recv()

    def pass_on(b, carry):
        own(b, 0, 0).wait_recv()
        forward(b, 0).start()
        own(b, 1, 1).wait_recv()
        forward(b, 1).start()
        return carry

    lax.fori_loop(0, NB, pass_on, 0)

    def finish(b, carry):
        own(b, 1, 0).wait_recv()
        own(b, 0, 1).wait_recv()
        for d in range(2):
            forward(b, d).wait_recv()
            for h in range(2):
                own(b, h, d).wait_send()
            forward(b, d).wait_send()
        return carry

    lax.fori_loop(0, NB, finish, 0)
    for copy in (*first, *rest, *r0, r1, *r2, *[step[2] for step in r3]):
        copy.wait_send()


def gather(w_down, avg_down, rw, gain):
    dma, any_, vmem = pltpu.SemaphoreType.DMA, pl.BlockSpec(memory_space=pl.ANY), pl.BlockSpec(memory_space=pltpu.VMEM)
    return pl.pallas_call(
        gather_kernel,
        out_shape=(
            pltpu.VMEM((ROWS, WIDE), BF16),
            pltpu.VMEM((ROWS, COLS), F32),
            pltpu.VMEM((1, ROWS), F32),
            pltpu.VMEM((NZ, NY * NC, WIDE), BF16),
        ),
        in_specs=[any_] * 4,
        out_specs=(vmem, vmem, vmem, vmem),
        scratch_shapes=[
            pltpu.VMEM((ROWS, COLS), F32),
            pltpu.VMEM((ROWS, COLS), F32),
            pltpu.VMEM((1, COLS), F32),
            pltpu.VMEM((1, COLS), F32),
            pltpu.VMEM((NX, 1, BLK), F32),
            pltpu.VMEM((NX, NB - 1, BLK), F32),
            pltpu.VMEM((NY * NC, NX, NX, 128), F32),
            pltpu.VMEM((NY * NC, WIDE), F32),
            dma((2, NB)),
            dma((2,)),
            dma((2, 3)),
            dma((2, 3)),
            dma((2, 2, NB)),
            dma((2, 2, NB)),
            dma((2, NB)),
            dma((2, NB)),
            dma((3,)),
            dma((3,)),
            dma,
            dma,
            dma((3,)),
            dma((3,)),
            dma((2, NZ // 2)),
            dma((2, NZ // 2)),
            pltpu.SemaphoreType.REGULAR,
        ],
        compiler_params=pltpu.CompilerParams(
            collective_id=0, has_side_effects=True, vmem_limit_bytes=24 << 20
        ),
        name="gather",
    )(*(pltpu.with_memory_space_constraint(v, pltpu.HBM) for v in (w_down, avg_down, rw, gain)))


PIECES = 8


def store_kernel(serve, fresh, scale, router, serve_out, fresh_out, scale_out, router_out, sem):
    copies = [
        pltpu.make_async_copy(scale, scale_out, sem.at[0]),
        pltpu.make_async_copy(router, router_out, sem.at[1]),
    ]
    n = ROWS // PIECES
    for k in range(PIECES):
        rows = pl.ds(k * n, n)
        copies.append(pltpu.make_async_copy(serve.at[rows], serve_out.at[rows], sem.at[2 + 2 * k]))
        copies.append(pltpu.make_async_copy(fresh.at[rows], fresh_out.at[rows], sem.at[3 + 2 * k]))
    for copy in copies:
        copy.start()
    for copy in copies:
        copy.wait()


def store(serve, fresh, scale, router):
    vmem, any_ = pl.BlockSpec(memory_space=pltpu.VMEM), pl.BlockSpec(memory_space=pl.ANY)
    return pl.pallas_call(
        store_kernel,
        out_shape=tuple(pltpu.HBM(v.shape, v.dtype) for v in (serve, fresh, scale, router)),
        in_specs=[vmem] * 4,
        out_specs=(any_,) * 4,
        scratch_shapes=[pltpu.SemaphoreType.DMA((2 + 2 * PIECES,))],
        compiler_params=pltpu.CompilerParams(vmem_limit_bytes=16 << 20),
        name="store",
    )(*(pltpu.with_memory_space_constraint(v, pltpu.VMEM) for v in (serve, fresh, scale, router)))


def body(w_down, avg_down, router_weight, router_gain):
    serve, fresh, scale, router = store(
        *gather(
            w_down.reshape(ROWS, COLS),
            avg_down.reshape(ROWS, COLS),
            router_weight.reshape(1, COLS),
            router_gain.reshape(1, COLS),
        )
    )
    return (
        serve.reshape(1, ROWS, WIDE),
        scale,
        router.reshape(NZ * NY * NC, WIDE).T,
        fresh.reshape(1, ROWS, COLS),
    )


def solution(mesh):
    placed = (P("ep", None, "fsdp"), P("ep", None, "fsdp"), P("fsdp", "ep"), P("fsdp"))
    return jax.shard_map(
        body,
        mesh=mesh,
        in_specs=placed,
        out_specs=(P("ep", None, None), P("ep", None), P(), P("ep", None, "fsdp")),
        check_vma=False,
    )
```

```python
import jax
import jax.numpy as jnp
from jax import lax
from jax.experimental import pallas as pl
from jax.experimental.pallas import tpu as pltpu
from jax.sharding import PartitionSpec as P

MESH = pl.DeviceIdType.MESH
F32, BF16 = jnp.float32, jnp.bfloat16
NX, NY, NZ, NC = 4, 4, 8, 2
ROWS, COLS = 1408, 512
WIDE = NX * COLS
HALF = COLS // 2
BLK = 128
NB = ROWS // BLK
EARLY = (40, 24)
NE = sum(EARLY)


def rows_of(b):
    return pl.ds(pl.multiple_of(b * BLK, BLK), BLK)


def gather_kernel(
    w_hbm, a_hbm, rw_hbm, gain_hbm, serve, fresh, scale, router,
    wbuf, abuf, rw, gain, m0, m1, early, piece, wide,
    load_sem, small_sem, m_send, m_recv, e_send, e_recv, own_send, own_recv, fwd_send, fwd_recv,
    r0_send, r0_recv, r1_send, r1_recv, r2_send, r2_recv, r3_send, r3_recv, greeted,
):
    x, e = lax.axis_index("fsdp"), lax.axis_index("ep")
    right, far, left = lax.rem(x + 1, NX), lax.rem(x + 2, NX), lax.rem(x + 3, NX)
    lo = lax.rem(e, NY * NC)
    z, y, c = e // (NY * NC), lo // NC, lax.rem(lo, NC)
    x_peers = ({"fsdp": right}, {"fsdp": left}, {"fsdp": far})
    mate = {"ep": e + 1 - 2 * c}
    y_up = {"ep": z * (NY * NC) + lax.rem(y + 1, NY) * NC + c}
    y_down = {"ep": z * (NY * NC) + lax.rem(y + NY - 1, NY) * NC + c}
    z_up = {"ep": lax.rem(z + 1, NZ) * (NY * NC) + lo}
    z_down = {"ep": lax.rem(z + NZ - 1, NZ) * (NY * NC) + lo}

    def load(b, k):
        src, dst = ((w_hbm, wbuf), (a_hbm, abuf))[k]
        return pltpu.make_async_copy(src.at[rows_of(b)], dst.at[rows_of(b)], load_sem.at[k, b])

    def start_load(b, carry):
        load(b, 0).start()
        load(b, 1).start()
        return carry

    def remote(src, dst, send, recv, peer):
        return pltpu.make_async_remote_copy(
            src_ref=src, dst_ref=dst, send_sem=send, recv_sem=recv, device_id=peer, device_id_type=MESH
        )

    small = [
        pltpu.make_async_copy(rw_hbm, rw, small_sem.at[0]),
        pltpu.make_async_copy(gain_hbm, gain, small_sem.at[1]),
    ]
    start_load(0, 0)
    for copy in small:
        copy.start()
    lax.fori_loop(1, NB, start_load, 0)

    barrier = pltpu.get_barrier_semaphore()
    for peer in x_peers:
        pl.semaphore_signal(barrier, inc=1, device_id=peer, device_id_type=MESH)
    links = (
        (c == 0, c == 1, mate),
        (y < NY - 1, y == NY - 1, y_up),
        (y == 0, y > 0, y_down),
        (z < NZ - 1, z == NZ - 1, z_up),
        (z == 0, z > 0, z_down),
    )
    entries, greetings = 3, 0
    for leads, follows, peer in links:
        entries += follows.astype(jnp.int32)
        greetings += leads.astype(jnp.int32)

        @pl.when(leads)
        def _(peer=peer):
            pl.semaphore_signal(barrier, inc=1, device_id=peer, device_id_type=MESH)

    def average(b):
        load(b, 0).wait()
        load(b, 1).wait()
        here = rows_of(b)
        top = None
        for k in range(COLS // 128):
            lanes = pl.ds(k * 128, 128)
            value = 0.5 * abuf[here, lanes] + 0.5 * wbuf[here, lanes]
            fresh[here, lanes] = value
            top = jnp.abs(value) if top is None else jnp.maximum(top, jnp.abs(value))
        return jnp.max(top.T, axis=0, keepdims=True)

    m0[x] = average(0)
    for copy in small:
        copy.wait()
    part = rw[...] * gain[...]
    for k in range(NX):
        piece[lo, x, k : k + 1, :] = part[:, k * 128 : (k + 1) * 128]
    pl.semaphore_wait(barrier, entries)
    for _, follows, peer in links:

        @pl.when(follows)
        def _(peer=peer):
            pl.semaphore_signal(greeted, inc=1, device_id=peer, device_id_type=MESH)


    first = [remote(m0.at[x], m0.at[x], m_send.at[0, k], m_recv.at[0, k], x_peers[k]) for k in range(3)]
    rest = [remote(m1.at[x], m1.at[x], m_send.at[1, k], m_recv.at[1, k], x_peers[k]) for k in range(3)]
    r0 = [remote(piece.at[lo, x], piece.at[lo, x], r0_send.at[k], r0_recv.at[k], x_peers[k]) for k in range(3)]
    for copy in first:
        copy.start()
    ahead = [
        [remote(fresh.at[rows], early.at[d, rows], e_send.at[d, k], e_recv.at[d, k], x_peers[d]) for d in range(2)]
        for k, rows in enumerate((pl.ds(0, EARLY[0]), pl.ds(EARLY[0], EARLY[1])))
    ]
    for copy in (*ahead[0], *r0):
        copy.start()

    def maxima(b, carry):
        m1[x, pl.ds(b - 1, 1), :] = average(b)
        return carry

    lax.fori_loop(1, NB, maxima, 0)
    for copy in (*rest, *ahead[1]):
        copy.start()

    mine = x * COLS

    def columns(start, width):
        return pl.ds(pl.multiple_of(start, 128), width)

    def rows_in(unit):
        if isinstance(unit, int) and unit < 2:
            return (pl.ds(0, NE), pl.ds(NE, BLK - NE))[unit]
        return rows_of(unit - 1)

    def own(unit, h, d):
        ref = serve.at[rows_in(unit), columns(mine + h * HALF, HALF)]
        return remote(ref, ref, own_send.at[d, h, unit - 1], own_recv.at[d, h, unit - 1], x_peers[d])

    def forward(unit, d):
        ref = serve.at[rows_in(unit), columns((left if d == 0 else right) * COLS + d * HALF, HALF)]
        return remote(ref, ref, fwd_send.at[d, unit], fwd_recv.at[d, unit], x_peers[d])

    def tall(top):
        return jnp.broadcast_to(top, (BLK, BLK)).T

    def narrow(src, here, start, scales):
        for k in range(COLS // 128):
            value = src[here, pl.ds(k * 128, 128)] / scales
            serve[here, columns(start + k * 128, 128)] = value.astype(BF16)

    for copy in first:
        copy.wait_recv()
    top = jnp.maximum(jnp.maximum(m0[0], m0[1]), jnp.maximum(m0[2], m0[3]))
    scale[:, 0:BLK] = top
    scales = tall(top)
    narrow(fresh, rows_in(1), mine, scales[NE:])
    for h, d in ((0, 0), (1, 1), (1, 0), (0, 1)):
        own(1, h, d).start()
    narrow(fresh, rows_in(0), mine, scales[:NE])
    for copy in rest:
        copy.wait_recv()

    def first_halves(b, carry):
        at = pl.ds(b - 1, 1)
        top = jnp.maximum(jnp.maximum(m1[0, at], m1[1, at]), jnp.maximum(m1[2, at], m1[3, at]))
        scale[:, columns(b * BLK, BLK)] = top
        narrow(fresh, rows_of(b), mine, tall(top))
        own(b + 1, 0, 0).start()
        own(b + 1, 1, 1).start()
        return carry

    def second_halves(b, carry):
        own(b + 1, 1, 0).start()
        own(b + 1, 0, 1).start()
        return carry

    lax.fori_loop(1, NB, first_halves, 0)
    lax.fori_loop(1, NB, second_halves, 0)

    scales = tall(scale[:, 0:BLK])
    for d, peer in ((0, left), (1, right)):
        ahead[0][d].wait_recv()
        ahead[1][d].wait_recv()
        narrow(early.at[d], rows_in(0), peer * COLS, scales[:NE])

    @pl.when(greetings > 0)
    def _():
        pl.semaphore_wait(greeted, greetings)

    for copy in r0:
        copy.wait_recv()
    r1 = remote(piece.at[lo], piece.at[lo], r1_send, r1_recv, mate)
    r1.start()
    r1.wait_recv()
    chip = piece.at[pl.ds(y * NC, NC)]
    below = piece.at[pl.ds(lax.rem(y + NY - 1, NY) * NC, NC)]
    r2 = [
        remote(chip, chip, r2_send.at[0], r2_recv.at[0], y_up),
        remote(chip, chip, r2_send.at[1], r2_recv.at[1], y_down),
        remote(below, below, r2_send.at[2], r2_recv.at[2], y_up),
    ]
    r2[0].start()
    r2[1].start()
    r2[0].wait_recv()
    r2[2].start()
    r2[1].wait_recv()
    r2[2].wait_recv()
    for i in range(NY * NC):
        for k in range(WIDE // 128):
            wide[i : i + 1, k * 128 : (k + 1) * 128] = piece[i, k // 4, k % 4 : k % 4 + 1, :]
    router[z] = wide[...].astype(BF16)
    r3 = []
    for k in range(NZ // 2):
        for d, peer in ((0, z_up), (1, z_down)):
            if d == 1 and k == NZ // 2 - 1:
                continue
            plane = router.at[lax.rem(z + (NZ - k if d == 0 else k), NZ)]
            r3.append((k, d, remote(plane, plane, r3_send.at[d, k], r3_recv.at[d, k], peer)))
    for k in range(NZ // 2):
        for step, d, copy in r3:
            if step == k:
                copy.start()
        for step, d, copy in r3:
            if step == k:
                copy.wait_recv()

    def pass_on(unit, carry=0):
        own(unit, 0, 0).wait_recv()
        forward(unit, 0).start()
        own(unit, 1, 1).wait_recv()
        forward(unit, 1).start()
        return carry

    forward(0, 0).start()
    forward(0, 1).start()
    pass_on(1)
    lax.fori_loop(2, NB + 1, pass_on, 0)

    def finish(unit, carry=0):
        own(unit, 1, 0).wait_recv()
        own(unit, 0, 1).wait_recv()
        for d in range(2):
            forward(unit, d).wait_recv()
            for h in range(2):
                own(unit, h, d).wait_send()
            forward(unit, d).wait_send()
        return carry

    for d in range(2):
        forward(0, d).wait_recv()
        forward(0, d).wait_send()
    finish(1)
    lax.fori_loop(2, NB + 1, finish, 0)
    for copy in (*first, *rest, *ahead[0], *ahead[1], *r0, r1, *r2, *[step[2] for step in r3]):
        copy.wait_send()


def gather(w_down, avg_down, rw, gain):
    dma, any_, vmem = pltpu.SemaphoreType.DMA, pl.BlockSpec(memory_space=pl.ANY), pl.BlockSpec(memory_space=pltpu.VMEM)
    return pl.pallas_call(
        gather_kernel,
        out_shape=(
            pltpu.VMEM((ROWS, WIDE), BF16),
            pltpu.VMEM((ROWS, COLS), F32),
            pltpu.VMEM((1, ROWS), F32),
            pltpu.VMEM((NZ, NY * NC, WIDE), BF16),
        ),
        in_specs=[any_] * 4,
        out_specs=(vmem, vmem, vmem, vmem),
        scratch_shapes=[
            pltpu.VMEM((ROWS, COLS), F32),
            pltpu.VMEM((ROWS, COLS), F32),
            pltpu.VMEM((1, COLS), F32),
            pltpu.VMEM((1, COLS), F32),
            pltpu.VMEM((NX, 1, BLK), F32),
            pltpu.VMEM((NX, NB - 1, BLK), F32),
            pltpu.VMEM((2, NE, COLS), F32),
            pltpu.VMEM((NY * NC, NX, NX, 128), F32),
            pltpu.VMEM((NY * NC, WIDE), F32),
            dma((2, NB)),
            dma((2,)),
            dma((2, 3)),
            dma((2, 3)),
            dma((2, 2)),
            dma((2, 2)),
            dma((2, 2, NB)),
            dma((2, 2, NB)),
            dma((2, NB + 1)),
            dma((2, NB + 1)),
            dma((3,)),
            dma((3,)),
            dma,
            dma,
            dma((3,)),
            dma((3,)),
            dma((2, NZ // 2)),
            dma((2, NZ // 2)),
            pltpu.SemaphoreType.REGULAR,
        ],
        compiler_params=pltpu.CompilerParams(
            collective_id=0, has_side_effects=True, vmem_limit_bytes=24 << 20
        ),
        name="gather",
    )(*(pltpu.with_memory_space_constraint(v, pltpu.HBM) for v in (w_down, avg_down, rw, gain)))


PIECES = 8


def store_kernel(serve, fresh, scale, router, serve_out, fresh_out, scale_out, router_out, sem):
    copies = [
        pltpu.make_async_copy(scale, scale_out, sem.at[0]),
        pltpu.make_async_copy(router, router_out, sem.at[1]),
    ]
    n = ROWS // PIECES
    for k in range(PIECES):
        rows = pl.ds(k * n, n)
        copies.append(pltpu.make_async_copy(serve.at[rows], serve_out.at[rows], sem.at[2 + 2 * k]))
        copies.append(pltpu.make_async_copy(fresh.at[rows], fresh_out.at[rows], sem.at[3 + 2 * k]))
    for copy in copies:
        copy.start()
    for copy in copies:
        copy.wait()


def store(serve, fresh, scale, router):
    vmem, any_ = pl.BlockSpec(memory_space=pltpu.VMEM), pl.BlockSpec(memory_space=pl.ANY)
    return pl.pallas_call(
        store_kernel,
        out_shape=tuple(pltpu.HBM(v.shape, v.dtype) for v in (serve, fresh, scale, router)),
        in_specs=[vmem] * 4,
        out_specs=(any_,) * 4,
        scratch_shapes=[pltpu.SemaphoreType.DMA((2 + 2 * PIECES,))],
        compiler_params=pltpu.CompilerParams(vmem_limit_bytes=16 << 20),
        name="store",
    )(*(pltpu.with_memory_space_constraint(v, pltpu.VMEM) for v in (serve, fresh, scale, router)))


def body(w_down, avg_down, router_weight, router_gain):
    serve, fresh, scale, router = store(
        *gather(
            w_down.reshape(ROWS, COLS),
            avg_down.reshape(ROWS, COLS),
            router_weight.reshape(1, COLS),
            router_gain.reshape(1, COLS),
        )
    )
    return (
        serve.reshape(1, ROWS, WIDE),
        scale,
        router.reshape(NZ * NY * NC, WIDE).T,
        fresh.reshape(1, ROWS, COLS),
    )


def solution(mesh):
    placed = (P("ep", None, "fsdp"), P("ep", None, "fsdp"), P("fsdp", "ep"), P("fsdp"))
    return jax.shard_map(
        body,
        mesh=mesh,
        in_specs=placed,
        out_specs=(P("ep", None, None), P("ep", None), P(), P("ep", None, "fsdp")),
        check_vma=False,
    )
```

```python
import jax
import jax.numpy as jnp
from jax import lax
from jax.experimental import pallas as pl
from jax.experimental.pallas import tpu as pltpu
from jax.sharding import PartitionSpec as P

MESH = pl.DeviceIdType.MESH
F32, BF16 = jnp.float32, jnp.bfloat16
NX, NY, NZ, NC = 4, 4, 8, 2
ROWS, COLS = 1408, 512
WIDE = NX * COLS
HALF = COLS // 2
BLK = 128
NB = ROWS // BLK
EARLY = (48, 16)
NE = sum(EARLY)


LOADS = (0, 256, 768, 1408)


def gather_kernel(
    w_hbm, a_hbm, rw_hbm, gain_hbm, serve, fresh, scale, router,
    buf, small, m0, m1, early, piece, wide,
    load_sem, small_sem, m_send, m_recv, e_send, e_recv, own_send, keep_recv, pass_recv, fwd_send, fwd_recv,
    r0_send, r0_recv, r12_send, r1_recv, r2_recv, r3_send, r3_recv, greeted,
):
    x, e = lax.axis_index("fsdp"), lax.axis_index("ep")
    right, far, left = lax.rem(x + 1, NX), lax.rem(x + 2, NX), lax.rem(x + 3, NX)
    lo = lax.rem(e, NY * NC)
    z, y, c = e // (NY * NC), lo // NC, lax.rem(lo, NC)
    x_peers = ({"fsdp": right}, {"fsdp": left}, {"fsdp": far})
    mate = {"ep": e + 1 - 2 * c}
    y_up = {"ep": z * (NY * NC) + lax.rem(y + 1, NY) * NC + c}
    y_down = {"ep": z * (NY * NC) + lax.rem(y + NY - 1, NY) * NC + c}
    z_up = {"ep": lax.rem(z + 1, NZ) * (NY * NC) + lo}
    z_down = {"ep": lax.rem(z + NZ - 1, NZ) * (NY * NC) + lo}

    barrier = pltpu.get_barrier_semaphore()
    for peer in (x_peers[2], x_peers[0], x_peers[1]):
        pl.semaphore_signal(barrier, inc=1, device_id=peer, device_id_type=MESH)

    def load(part, k):
        rows = pl.ds(LOADS[part], LOADS[part + 1] - LOADS[part])
        return pltpu.make_async_copy((w_hbm, a_hbm)[k].at[rows], buf.at[k, rows], load_sem.at[part])

    def wait_for(ref, sem):
        pltpu.make_async_copy(ref, ref, sem).wait()

    def loaded(part):
        wait_for(buf.at[:, pl.ds(LOADS[part], LOADS[part + 1] - LOADS[part])], load_sem.at[part])

    def remote(src, dst, send, recv, peer):
        return pltpu.make_async_remote_copy(
            src_ref=src, dst_ref=dst, send_sem=send, recv_sem=recv, device_id=peer, device_id_type=MESH
        )

    for part in range(len(LOADS) - 1):
        load(part, 0).start()
        load(part, 1).start()
        if part == 0:
            pltpu.make_async_copy(rw_hbm, small.at[0], small_sem).start()
            pltpu.make_async_copy(gain_hbm, small.at[1], small_sem).start()

    links = (
        (c == 1, c == 0, mate),
        (y < NY - 1, y == NY - 1, y_up),
        (y == 0, y > 0, y_down),
        (z < NZ - 1, z == NZ - 1, z_up),
        (z == 0, z > 0, z_down),
    )
    entries, greetings = 3, 0
    for leads, follows, peer in links:
        entries += follows.astype(jnp.int32)
        greetings += leads.astype(jnp.int32)

        @pl.when(leads)
        def _(peer=peer):
            pl.semaphore_signal(barrier, inc=1, device_id=peer, device_id_type=MESH)

    def rows_of(b):
        return pl.ds(pl.multiple_of(b * BLK, BLK), BLK)

    def columns(start, width):
        return pl.ds(pl.multiple_of(start, 128), width)

    def average(b):
        here = rows_of(b)
        top = None
        for k in range(COLS // 128):
            lanes = pl.ds(k * 128, 128)
            value = 0.5 * buf[1, here, lanes] + 0.5 * buf[0, here, lanes]
            fresh[here, lanes] = value
            top = jnp.abs(value) if top is None else jnp.maximum(top, jnp.abs(value))
        return jnp.max(top.T, axis=0, keepdims=True)

    loaded(0)
    for b in range(2):
        m0[x, b : b + 1, :] = average(b)
    pl.semaphore_wait(barrier, entries)

    for k in (2, 0, 1):
        remote(m0.at[x], m0.at[x], m_send.at[0], m_recv.at[0], x_peers[k]).start()
    ahead = (pl.ds(0, EARLY[0]), pl.ds(EARLY[0], EARLY[1]))
    for d in range(2):
        remote(fresh.at[ahead[0]], early.at[d, ahead[0]], e_send, e_recv, x_peers[d]).start()
    wait_for(small, small_sem)
    part = small[0] * small[1]
    for k in range(NX):
        piece[lo, x, k : k + 1, :] = part[:, k * 128 : (k + 1) * 128]
    for k in range(3):
        remote(piece.at[lo, x], piece.at[lo, x], r0_send, r0_recv, x_peers[k]).start()
    for _, follows, peer in links:

        @pl.when(follows)
        def _(peer=peer):
            pl.semaphore_signal(greeted, inc=1, device_id=peer, device_id_type=MESH)

    def maxima(b, carry):
        m1[x, pl.ds(b - 2, 1), :] = average(b)
        return carry

    for part in range(1, len(LOADS) - 1):
        loaded(part)
        lax.fori_loop(LOADS[part] // BLK, LOADS[part + 1] // BLK, maxima, 0)
    for k in (2, 0, 1):
        remote(m1.at[x], m1.at[x], m_send.at[1], m_recv.at[1], x_peers[k]).start()
    for d in range(2):
        remote(fresh.at[ahead[1]], early.at[d, ahead[1]], e_send, e_recv, x_peers[d]).start()

    mine = x * COLS

    def tall(top):
        return jnp.broadcast_to(top, (BLK, BLK)).T

    def narrow(src, here, start, scales):
        for k in range(COLS // 128):
            value = src[here, pl.ds(k * 128, 128)] / scales
            serve[here, columns(start + k * 128, 128)] = value.astype(BF16)

    def own(rows, h, d):
        ref = serve.at[rows, columns(mine + h * HALF, HALF)]
        return remote(ref, ref, own_send, pass_recv.at[d] if h == d else keep_recv, x_peers[d])

    def forward(d):
        ref = serve.at[:, columns((left if d == 0 else right) * COLS + d * HALF, HALF)]
        return remote(ref, ref, fwd_send, fwd_recv, x_peers[d])

    wait_for(m0.at[pl.ds(0, 3)], m_recv.at[0])
    top = jnp.maximum(jnp.maximum(m0[0], m0[1]), jnp.maximum(m0[2], m0[3]))
    scale[:, 0:BLK] = top[0:1]
    scale[:, BLK : 2 * BLK] = top[1:2]
    scales = tall(top[0:1])
    narrow(fresh, pl.ds(NE, BLK - NE), mine, scales[NE:])
    narrow(fresh, rows_of(1), mine, tall(top[1:2]))
    for h, d in ((0, 0), (1, 1), (1, 0), (0, 1)):
        own(pl.ds(NE, 2 * BLK - NE), h, d).start()
    narrow(fresh, pl.ds(0, NE), mine, scales[:NE])
    wait_for(m1.at[pl.ds(0, 3)], m_recv.at[1])

    def narrowed(b, carry):
        at = pl.ds(b - 2, 1)
        top = jnp.maximum(jnp.maximum(m1[0, at], m1[1, at]), jnp.maximum(m1[2, at], m1[3, at]))
        scale[:, columns(b * BLK, BLK)] = top
        narrow(fresh, rows_of(b), mine, tall(top))
        return carry

    lax.fori_loop(2, NB, narrowed, 0)
    for h, d in ((0, 0), (1, 1), (1, 0), (0, 1)):
        own(pl.ds(2 * BLK, ROWS - 2 * BLK), h, d).start()

    wait_for(early, e_recv)
    scales = tall(scale[:, 0:BLK])
    for d, peer in ((0, left), (1, right)):
        narrow(early.at[d], pl.ds(0, NE), peer * COLS, scales[:NE])

    @pl.when(greetings > 0)
    def _():
        pl.semaphore_wait(greeted, greetings)

    wait_for(piece.at[lo, pl.ds(0, 3)], r0_recv)
    remote(piece.at[lo], piece.at[lo], r12_send, r1_recv, mate).start()
    chip = piece.at[pl.ds(y * NC, NC)]
    below = piece.at[pl.ds(lax.rem(y + NY - 1, NY) * NC, NC)]
    wait_for(piece.at[0], r1_recv)
    remote(chip, chip, r12_send, r2_recv.at[0], y_up).start()
    remote(chip, chip, r12_send, r2_recv.at[1], y_down).start()
    wait_for(chip, r2_recv.at[0])
    remote(below, below, r12_send, r2_recv.at[1], y_up).start()
    wait_for(piece.at[pl.ds(0, 2 * NC)], r2_recv.at[1])
    for i in range(NY * NC):
        for k in range(WIDE // 128):
            wide[i : i + 1, k * 128 : (k + 1) * 128] = piece[i, k // 4, k % 4 : k % 4 + 1, :]
    router[z] = wide[...].astype(BF16)

    def z_step(k):
        for d, peer in ((0, z_up), (1, z_down)):
            if d == 0 or k < NZ // 2 - 1:
                plane = router.at[lax.rem(z + (NZ - k if d == 0 else k), NZ)]
                remote(plane, plane, r3_send, r3_recv.at[k], peer).start()

    def z_arrived(k):
        wait_for(router.at[pl.ds(0, 2 if k < NZ // 2 - 1 else 1)], r3_recv.at[k])

    z_step(0)
    for d in range(2):
        wait_for(serve.at[pl.ds(NE, ROWS - NE), columns(0, HALF)], pass_recv.at[d])
        forward(d).start()
    for k in range(1, NZ // 2):
        z_arrived(k - 1)
        z_step(k)
    z_arrived(NZ // 2 - 1)

    wait_for(early, e_send)
    for k, m in enumerate((m0, m1)):
        wait_for(m.at[pl.ds(0, 3)], m_send.at[k])
    wait_for(piece.at[0, pl.ds(0, 3)], r0_send)
    wait_for(piece.at[pl.ds(0, 1 + 3 * NC)], r12_send)
    wait_for(router.at[pl.ds(0, NZ - 1)], r3_send)
    wait_for(serve.at[pl.ds(NE, ROWS - NE), columns(0, COLS)], keep_recv)
    wait_for(serve.at[pl.ds(NE, ROWS - NE), columns(0, 2 * COLS)], own_send)
    wait_for(serve.at[:, columns(0, COLS)], fwd_send)
    wait_for(serve.at[:, columns(0, COLS)], fwd_recv)


def gather(w_down, avg_down, rw, gain):
    dma, any_, vmem = pltpu.SemaphoreType.DMA, pl.BlockSpec(memory_space=pl.ANY), pl.BlockSpec(memory_space=pltpu.VMEM)
    return pl.pallas_call(
        gather_kernel,
        out_shape=(
            pltpu.VMEM((ROWS, WIDE), BF16),
            pltpu.VMEM((ROWS, COLS), F32),
            pltpu.VMEM((1, ROWS), F32),
            pltpu.VMEM((NZ, NY * NC, WIDE), BF16),
        ),
        in_specs=[any_] * 4,
        out_specs=(vmem, vmem, vmem, vmem),
        scratch_shapes=[
            pltpu.VMEM((2, ROWS, COLS), F32),
            pltpu.VMEM((2, 1, COLS), F32),
            pltpu.VMEM((NX, 2, BLK), F32),
            pltpu.VMEM((NX, NB - 2, BLK), F32),
            pltpu.VMEM((2, NE, COLS), F32),
            pltpu.VMEM((NY * NC, NX, NX, 128), F32),
            pltpu.VMEM((NY * NC, WIDE), F32),
            dma((len(LOADS) - 1,)),
            dma,
            dma((2,)),
            dma((2,)),
            dma,
            dma,
            dma,
            dma,
            dma((2,)),
            dma,
            dma,
            dma,
            dma,
            dma,
            dma,
            dma((2,)),
            dma,
            dma((NZ // 2,)),
            pltpu.SemaphoreType.REGULAR,
        ],
        compiler_params=pltpu.CompilerParams(
            collective_id=0, has_side_effects=True, vmem_limit_bytes=24 << 20
        ),
        name="gather",
    )(*(pltpu.with_memory_space_constraint(v, pltpu.HBM) for v in (w_down, avg_down, rw, gain)))


def store_kernel(serve, fresh, scale, router, serve_out, fresh_out, scale_out, router_out, sem):
    pairs = ((serve, serve_out), (fresh, fresh_out), (router, router_out), (scale, scale_out))
    copies = [pltpu.make_async_copy(src, dst, sem.at[k]) for k, (src, dst) in enumerate(pairs)]
    for copy in copies:
        copy.start()
    for copy in copies:
        copy.wait()


def store(serve, fresh, scale, router):
    vmem, any_ = pl.BlockSpec(memory_space=pltpu.VMEM), pl.BlockSpec(memory_space=pl.ANY)
    return pl.pallas_call(
        store_kernel,
        out_shape=tuple(pltpu.HBM(v.shape, v.dtype) for v in (serve, fresh, scale, router)),
        in_specs=[vmem] * 4,
        out_specs=(any_,) * 4,
        scratch_shapes=[pltpu.SemaphoreType.DMA((4,))],
        compiler_params=pltpu.CompilerParams(vmem_limit_bytes=16 << 20),
        name="store",
    )(*(pltpu.with_memory_space_constraint(v, pltpu.VMEM) for v in (serve, fresh, scale, router)))


def body(w_down, avg_down, router_weight, router_gain):
    serve, fresh, scale, router = store(
        *gather(
            w_down.reshape(ROWS, COLS),
            avg_down.reshape(ROWS, COLS),
            router_weight.reshape(1, COLS),
            router_gain.reshape(1, COLS),
        )
    )
    return (
        serve.reshape(1, ROWS, WIDE),
        scale,
        router.reshape(NZ * NY * NC, WIDE).T,
        fresh.reshape(1, ROWS, COLS),
    )


def solution(mesh):
    placed = (P("ep", None, "fsdp"), P("ep", None, "fsdp"), P("fsdp", "ep"), P("fsdp"))
    return jax.shard_map(
        body,
        mesh=mesh,
        in_specs=placed,
        out_specs=(P("ep", None, None), P("ep", None), P(), P("ep", None, "fsdp")),
        check_vma=False,
    )
```

```python
import jax
import jax.numpy as jnp
from jax import lax
from jax.experimental import pallas as pl
from jax.experimental.pallas import tpu as pltpu
from jax.sharding import PartitionSpec as P

MESH = pl.DeviceIdType.MESH
F32, BF16 = jnp.float32, jnp.bfloat16
NX, NY, NZ, NC = 4, 4, 8, 2
ROWS, COLS = 1408, 512
WIDE = NX * COLS
HALF = COLS // 2
BLK = 128
NB = ROWS // BLK
NE = 48


RS = (1232, 800)
REST = ROWS - min(RS)
LOADS = (0, 256, 768, 1408)


def gather_kernel(
    w_hbm, a_hbm, rw_hbm, gain_hbm, serve, fresh, scale, router,
    buf, small, m0, m1, early, piece, wide,
    load_sem, small_sem, m_send, m_recv, e_send, e_recv, own_send, keep_recv, pass_recv, fwd_send, fwd_recv,
    r0_send, r0_recv, r12_send, r1_recv, r2_recv, r3_send, r3_recv, greeted,
):
    x, e = lax.axis_index("fsdp"), lax.axis_index("ep")
    right, far, left = lax.rem(x + 1, NX), lax.rem(x + 2, NX), lax.rem(x + 3, NX)
    lo = lax.rem(e, NY * NC)
    z, y, c = e // (NY * NC), lo // NC, lax.rem(lo, NC)
    x_peers = ({"fsdp": right}, {"fsdp": left}, {"fsdp": far})
    mate = {"ep": e + 1 - 2 * c}
    y_up = {"ep": z * (NY * NC) + lax.rem(y + 1, NY) * NC + c}
    y_down = {"ep": z * (NY * NC) + lax.rem(y + NY - 1, NY) * NC + c}
    z_up = {"ep": lax.rem(z + 1, NZ) * (NY * NC) + lo}
    z_down = {"ep": lax.rem(z + NZ - 1, NZ) * (NY * NC) + lo}

    barrier = pltpu.get_barrier_semaphore()
    for peer in (x_peers[2], x_peers[0], x_peers[1]):
        pl.semaphore_signal(barrier, inc=1, device_id=peer, device_id_type=MESH)

    def load(part, k):
        rows = pl.ds(LOADS[part], LOADS[part + 1] - LOADS[part])
        return pltpu.make_async_copy((w_hbm, a_hbm)[k].at[rows], buf.at[k, rows], load_sem.at[part])

    def wait_for(ref, sem):
        pltpu.make_async_copy(ref, ref, sem).wait()

    def loaded(part):
        wait_for(buf.at[:, pl.ds(LOADS[part], LOADS[part + 1] - LOADS[part])], load_sem.at[part])

    def remote(src, dst, send, recv, peer):
        return pltpu.make_async_remote_copy(
            src_ref=src, dst_ref=dst, send_sem=send, recv_sem=recv, device_id=peer, device_id_type=MESH
        )

    for part in range(len(LOADS) - 1):
        load(part, 0).start()
        load(part, 1).start()
        if part == 0:
            pltpu.make_async_copy(rw_hbm, small.at[0], small_sem).start()
            pltpu.make_async_copy(gain_hbm, small.at[1], small_sem).start()

    links = (
        (c == 1, c == 0, mate),
        (y < NY - 1, y == NY - 1, y_up),
        (y == 0, y > 0, y_down),
        (z < NZ - 1, z == NZ - 1, z_up),
        (z == 0, z > 0, z_down),
    )
    entries, greetings = 3, 0
    for leads, follows, peer in links:
        entries += follows.astype(jnp.int32)
        greetings += leads.astype(jnp.int32)

        @pl.when(leads)
        def _(peer=peer):
            pl.semaphore_signal(barrier, inc=1, device_id=peer, device_id_type=MESH)

    def rows_of(b):
        return pl.ds(pl.multiple_of(b * BLK, BLK), BLK)

    def columns(start, width):
        return pl.ds(pl.multiple_of(start, 128), width)

    def average(b):
        here = rows_of(b)
        top = None
        for k in range(COLS // 128):
            lanes = pl.ds(k * 128, 128)
            value = 0.5 * buf[1, here, lanes] + 0.5 * buf[0, here, lanes]
            fresh[here, lanes] = value
            top = jnp.abs(value) if top is None else jnp.maximum(top, jnp.abs(value))
        return jnp.max(top.T, axis=0, keepdims=True)

    loaded(0)
    for b in range(2):
        m0[x, b : b + 1, :] = average(b)
    pl.semaphore_wait(barrier, entries)

    for k in (2, 0, 1):
        remote(m0.at[x], m0.at[x], m_send.at[0], m_recv.at[0], x_peers[k]).start()
    for d in range(2):
        remote(fresh.at[pl.ds(0, NE)], early.at[d], e_send, e_recv, x_peers[d]).start()
    wait_for(small, small_sem)
    part = small[0] * small[1]
    for k in range(NX):
        piece[lo, x, k : k + 1, :] = part[:, k * 128 : (k + 1) * 128]
    for k in range(3):
        remote(piece.at[lo, x], piece.at[lo, x], r0_send, r0_recv, x_peers[k]).start()
    for _, follows, peer in links:

        @pl.when(follows)
        def _(peer=peer):
            pl.semaphore_signal(greeted, inc=1, device_id=peer, device_id_type=MESH)

    def maxima(b, carry):
        m1[x, pl.ds(b - 2, 1), :] = average(b)
        return carry

    for part in range(1, len(LOADS) - 1):
        loaded(part)
        lax.fori_loop(LOADS[part] // BLK, LOADS[part + 1] // BLK, maxima, 0)
    for k in (2, 0, 1):
        remote(m1.at[x], m1.at[x], m_send.at[1], m_recv.at[1], x_peers[k]).start()

    mine = x * COLS

    def tall(top):
        return jnp.broadcast_to(top, (BLK, BLK)).T

    def narrow(src, here, start, scales):
        for k in range(COLS // 128):
            value = src[here, pl.ds(k * 128, 128)] / scales
            serve[here, columns(start + k * 128, 128)] = value.astype(BF16)

    def own(rows, h, d):
        ref = serve.at[rows, columns(mine + h * HALF, HALF)]
        return remote(ref, ref, own_send, pass_recv.at[d] if h == d else keep_recv, x_peers[d])

    def forward(n, d):
        ref = serve.at[pl.ds(0, n), columns((left if d == 0 else right) * COLS + d * HALF, HALF)]
        return remote(ref, ref, fwd_send, fwd_recv, x_peers[d])

    def by_core(do):
        for core, n in enumerate(RS):
            pl.when(c == core)(lambda n=n: do(n))

    chip = piece.at[pl.ds(y * NC, NC)]
    below = piece.at[pl.ds(lax.rem(y + NY - 1, NY) * NC, NC)]

    def z_step(k):
        for d, peer in ((0, z_up), (1, z_down)):
            if d == 0 or k < NZ // 2 - 1:
                plane = router.at[lax.rem(z + (NZ - k if d == 0 else k), NZ)]
                remote(plane, plane, r3_send, r3_recv.at[k], peer).start()

    def z_arrived(k):
        wait_for(router.at[pl.ds(0, 2 if k < NZ // 2 - 1 else 1)], r3_recv.at[k])

    wait_for(m0.at[pl.ds(0, 3)], m_recv.at[0])
    top = jnp.maximum(jnp.maximum(m0[0], m0[1]), jnp.maximum(m0[2], m0[3]))
    scale[:, 0:BLK] = top[0:1]
    scale[:, BLK : 2 * BLK] = top[1:2]
    scales = tall(top[0:1])
    narrow(fresh, pl.ds(NE, BLK - NE), mine, scales[NE:])
    narrow(fresh, rows_of(1), mine, tall(top[1:2]))
    for h, d in ((0, 0), (1, 1), (1, 0), (0, 1)):
        own(pl.ds(NE, 2 * BLK - NE), h, d).start()
    narrow(fresh, pl.ds(0, NE), mine, scales[:NE])

    @pl.when(greetings > 0)
    def _():
        pl.semaphore_wait(greeted, greetings)

    wait_for(piece.at[lo, pl.ds(0, 3)], r0_recv)
    remote(piece.at[lo], piece.at[lo], r12_send, r1_recv, mate).start()
    wait_for(m1.at[pl.ds(0, 3)], m_recv.at[1])

    def narrowed(b, carry):
        at = pl.ds(b - 2, 1)
        top = jnp.maximum(jnp.maximum(m1[0, at], m1[1, at]), jnp.maximum(m1[2, at], m1[3, at]))
        scale[:, columns(b * BLK, BLK)] = top
        narrow(fresh, rows_of(b), mine, tall(top))
        return carry

    lax.fori_loop(2, NB, narrowed, 0)

    @by_core
    def _(n):
        for h, d in ((0, 0), (1, 1), (1, 0), (0, 1)):
            own(pl.ds(2 * BLK, n - 2 * BLK), h, d).start()

    wait_for(piece.at[0], r1_recv)
    remote(chip, chip, r12_send, r2_recv.at[0], y_up).start()
    remote(chip, chip, r12_send, r2_recv.at[1], y_down).start()

    wait_for(early, e_recv)
    scales = tall(scale[:, 0:BLK])
    for d, peer in ((0, left), (1, right)):
        narrow(early.at[d], pl.ds(0, NE), peer * COLS, scales[:NE])

    wait_for(chip, r2_recv.at[0])
    remote(below, below, r12_send, r2_recv.at[1], y_up).start()
    wait_for(piece.at[pl.ds(0, 2 * NC)], r2_recv.at[1])
    for i in range(NY * NC):
        for k in range(WIDE // 128):
            wide[i : i + 1, k * 128 : (k + 1) * 128] = piece[i, k // 4, k % 4 : k % 4 + 1, :]
    router[z] = wide[...].astype(BF16)
    z_step(0)
    if NZ > 2:
        z_arrived(0)
        z_step(1)

    @by_core
    def _(n):
        for d in range(2):
            wait_for(serve.at[pl.ds(NE, n - NE), columns(0, HALF)], pass_recv.at[d])
            forward(n, d).start()

    for k in range(2, NZ // 2):
        z_arrived(k - 1)
        z_step(k)
    z_arrived(NZ // 2 - 1)

    wait_for(early, e_send)
    for k, m in enumerate((m0, m1)):
        wait_for(m.at[pl.ds(0, 3)], m_send.at[k])
    wait_for(piece.at[0, pl.ds(0, 3)], r0_send)
    wait_for(piece.at[pl.ds(0, 1 + 3 * NC)], r12_send)
    wait_for(router.at[pl.ds(0, NZ - 1)], r3_send)

    @by_core
    def _(n):
        wait_for(serve.at[pl.ds(NE, n - NE), columns(0, COLS)], keep_recv)
        wait_for(serve.at[pl.ds(NE, n - NE), columns(0, 2 * COLS)], own_send)
        wait_for(serve.at[pl.ds(0, n), columns(0, COLS)], fwd_send)
        wait_for(serve.at[pl.ds(0, n), columns(0, COLS)], fwd_recv)


def rest_kernel(serve, stored, rest, own_send, keep_recv, pass_recv, fwd_send, fwd_recv):
    x, c = lax.axis_index("fsdp"), lax.rem(lax.axis_index("ep"), NC)
    right, left = lax.rem(x + 1, NX), lax.rem(x + 3, NX)
    peers = ({"fsdp": right}, {"fsdp": left})
    barrier = pltpu.get_barrier_semaphore()
    for peer in peers:
        pl.semaphore_signal(barrier, inc=1, device_id=peer, device_id_type=MESH)
    pl.semaphore_wait(barrier, 2)

    def columns(start, width):
        return pl.ds(pl.multiple_of(start, 128), width)

    def wait_for(n, width, sem):
        ref = rest.at[pl.ds(0, n), columns(0, width)]
        pltpu.make_async_copy(ref, ref, sem).wait()

    def remote(src, dst, send, recv, d):
        return pltpu.make_async_remote_copy(
            src_ref=src, dst_ref=dst, send_sem=send, recv_sem=recv, device_id=peers[d], device_id_type=MESH
        )

    def gather_rest(first):
        n = ROWS - first
        for h, d in ((0, 0), (1, 1), (1, 0), (0, 1)):
            lanes = columns(x * COLS + h * HALF, HALF)
            src, dst = serve.at[pl.ds(first, n), lanes], rest.at[pl.ds(0, n), lanes]
            remote(src, dst, own_send, pass_recv.at[d] if h == d else keep_recv, d).start()
        for d, source in ((0, left), (1, right)):
            wait_for(n, HALF, pass_recv.at[d])
            ref = rest.at[pl.ds(0, n), columns(source * COLS + d * HALF, HALF)]
            remote(ref, ref, fwd_send, fwd_recv, d).start()
        wait_for(n, 2 * HALF, keep_recv)
        wait_for(n, 4 * HALF, own_send)
        wait_for(n, 2 * HALF, fwd_send)
        wait_for(n, 2 * HALF, fwd_recv)

    for core, first in enumerate(RS):
        pl.when(c == core)(lambda first=first: gather_rest(first))


def gather(w_down, avg_down, rw, gain):
    dma, any_, vmem = pltpu.SemaphoreType.DMA, pl.BlockSpec(memory_space=pl.ANY), pl.BlockSpec(memory_space=pltpu.VMEM)
    return pl.pallas_call(
        gather_kernel,
        out_shape=(
            pltpu.VMEM((ROWS, WIDE), BF16),
            pltpu.VMEM((ROWS, COLS), F32),
            pltpu.VMEM((1, ROWS), F32),
            pltpu.VMEM((NZ, NY * NC, WIDE), BF16),
        ),
        in_specs=[any_] * 4,
        out_specs=(vmem, vmem, vmem, vmem),
        scratch_shapes=[
            pltpu.VMEM((2, ROWS, COLS), F32),
            pltpu.VMEM((2, 1, COLS), F32),
            pltpu.VMEM((NX, 2, BLK), F32),
            pltpu.VMEM((NX, NB - 2, BLK), F32),
            pltpu.VMEM((2, NE, COLS), F32),
            pltpu.VMEM((NY * NC, NX, NX, 128), F32),
            pltpu.VMEM((NY * NC, WIDE), F32),
            dma((len(LOADS) - 1,)),
            dma,
            dma((2,)),
            dma((2,)),
            dma,
            dma,
            dma,
            dma,
            dma((2,)),
            dma,
            dma,
            dma,
            dma,
            dma,
            dma,
            dma((2,)),
            dma,
            dma((NZ // 2,)),
            pltpu.SemaphoreType.REGULAR,
        ],
        compiler_params=pltpu.CompilerParams(
            collective_id=0, has_side_effects=True, vmem_limit_bytes=24 << 20
        ),
        name="gather",
    )(*(pltpu.with_memory_space_constraint(v, pltpu.HBM) for v in (w_down, avg_down, rw, gain)))


def gather_rest(serve, stored):
    dma, any_, vmem = pltpu.SemaphoreType.DMA, pl.BlockSpec(memory_space=pl.ANY), pl.BlockSpec(memory_space=pltpu.VMEM)
    return pl.pallas_call(
        rest_kernel,
        out_shape=pltpu.VMEM((REST, WIDE), BF16),
        in_specs=[vmem, any_],
        out_specs=vmem,
        scratch_shapes=[dma, dma, dma((2,)), dma, dma],
        compiler_params=pltpu.CompilerParams(
            collective_id=1, has_side_effects=True, vmem_limit_bytes=8 << 20
        ),
        name="gather_rest",
    )(pltpu.with_memory_space_constraint(serve, pltpu.VMEM), pltpu.with_memory_space_constraint(stored, pltpu.HBM))


def store_kernel(serve, fresh, scale, router, serve_out, fresh_out, scale_out, router_out, stored, sem):
    x, c = lax.axis_index("fsdp"), lax.rem(lax.axis_index("ep"), NC)
    mine = pl.ds(pl.multiple_of(x * COLS, COLS), COLS)

    def store_first(n):
        left = pl.ds(n, ROWS - n)
        copies = [
            pltpu.make_async_copy(fresh, fresh_out, sem.at[0]),
            pltpu.make_async_copy(scale, scale_out, sem.at[1]),
            pltpu.make_async_copy(router, router_out, sem.at[2]),
            pltpu.make_async_copy(serve.at[pl.ds(0, n)], serve_out.at[pl.ds(0, n)], sem.at[3]),
            pltpu.make_async_copy(serve.at[left, mine], serve_out.at[left, mine], sem.at[4]),
        ]
        for copy in copies:
            copy.start()
        for copy in copies:
            copy.wait()

    for core, n in enumerate(RS):
        pl.when(c == core)(lambda n=n: store_first(n))


def store(serve, fresh, scale, router):
    vmem, any_ = pl.BlockSpec(memory_space=pltpu.VMEM), pl.BlockSpec(memory_space=pl.ANY)
    return pl.pallas_call(
        store_kernel,
        out_shape=(*(pltpu.HBM(v.shape, v.dtype) for v in (serve, fresh, scale, router)), pltpu.HBM((8, 128), F32)),
        in_specs=[vmem] * 4,
        out_specs=(any_,) * 5,
        scratch_shapes=[pltpu.SemaphoreType.DMA((5,))],
        compiler_params=pltpu.CompilerParams(vmem_limit_bytes=16 << 20),
        name="store",
    )(*(pltpu.with_memory_space_constraint(v, pltpu.VMEM) for v in (serve, fresh, scale, router)))


def store_rest_kernel(rest, serve_in, serve_out, sem):
    x, c = lax.axis_index("fsdp"), lax.rem(lax.axis_index("ep"), NC)

    def store_last(first):
        n = ROWS - first
        copies = []
        for k in range(1, NX):
            lanes = pl.ds(pl.multiple_of(lax.rem(x + k, NX) * COLS, COLS), COLS)
            src, dst = rest.at[pl.ds(0, n), lanes], serve_out.at[pl.ds(first, n), lanes]
            copies.append(pltpu.make_async_copy(src, dst, sem.at[k - 1]))
        for copy in copies:
            copy.start()
        for copy in copies:
            copy.wait()

    for core, first in enumerate(RS):
        pl.when(c == core)(lambda first=first: store_last(first))


def store_rest(rest, serve):
    vmem, any_ = pl.BlockSpec(memory_space=pltpu.VMEM), pl.BlockSpec(memory_space=pl.ANY)
    return pl.pallas_call(
        store_rest_kernel,
        out_shape=pltpu.HBM(serve.shape, serve.dtype),
        in_specs=[vmem, any_],
        out_specs=any_,
        input_output_aliases={1: 0},
        scratch_shapes=[pltpu.SemaphoreType.DMA((NX - 1,))],
        compiler_params=pltpu.CompilerParams(vmem_limit_bytes=8 << 20),
        name="store_rest",
    )(pltpu.with_memory_space_constraint(rest, pltpu.VMEM), pltpu.with_memory_space_constraint(serve, pltpu.HBM))


def body(w_down, avg_down, router_weight, router_gain):
    gathered, fresh, scale, router = gather(
        w_down.reshape(ROWS, COLS),
        avg_down.reshape(ROWS, COLS),
        router_weight.reshape(1, COLS),
        router_gain.reshape(1, COLS),
    )
    serve, fresh, scale, router, stored = store(gathered, fresh, scale, router)
    serve = store_rest(gather_rest(gathered, stored), serve)
    return (
        serve.reshape(1, ROWS, WIDE),
        scale,
        router.reshape(NZ * NY * NC, WIDE).T,
        fresh.reshape(1, ROWS, COLS),
    )


def solution(mesh):
    placed = (P("ep", None, "fsdp"), P("ep", None, "fsdp"), P("fsdp", "ep"), P("fsdp"))
    return jax.shard_map(
        body,
        mesh=mesh,
        in_specs=placed,
        out_specs=(P("ep", None, None), P("ep", None), P(), P("ep", None, "fsdp")),
        check_vma=False,
    )
```

```python
import jax
import jax.numpy as jnp
from jax import lax
from jax.experimental import pallas as pl
from jax.experimental.pallas import tpu as pltpu
from jax.sharding import PartitionSpec as P

MESH = pl.DeviceIdType.MESH
F32, BF16 = jnp.float32, jnp.bfloat16
NX, NY, NZ, NC = 4, 4, 8, 2
ROWS, COLS = 1408, 512
WIDE = NX * COLS
HALF = COLS // 2
BLK = 128
NB = ROWS // BLK
NE = 48


RS = (1072, 736)
REST = ROWS - min(RS)
LOADS = (0, 256, 768, 1408)


def gather_kernel(
    w_hbm, a_hbm, rw_hbm, gain_hbm, serve, fresh, scale, router,
    buf, small, m0, m1, early, piece, wide,
    load_sem, small_sem, m_send, m_recv, e_send, e_recv, own_send, keep_recv, pass_recv, fwd_send, fwd_recv,
    r0_send, r0_recv, r12_send, r1_recv, r2_recv, r3_send, r3_recv, greeted,
):
    x, e = lax.axis_index("fsdp"), lax.axis_index("ep")
    right, far, left = lax.rem(x + 1, NX), lax.rem(x + 2, NX), lax.rem(x + 3, NX)
    lo = lax.rem(e, NY * NC)
    z, y, c = e // (NY * NC), lo // NC, lax.rem(lo, NC)
    x_peers = ({"fsdp": right}, {"fsdp": left}, {"fsdp": far})
    mate = {"ep": e + 1 - 2 * c}
    y_up = {"ep": z * (NY * NC) + lax.rem(y + 1, NY) * NC + c}
    y_down = {"ep": z * (NY * NC) + lax.rem(y + NY - 1, NY) * NC + c}

    def z_peer(hop):
        return {"ep": lax.rem(z + NZ + hop, NZ) * (NY * NC) + lo}


    barrier = pltpu.get_barrier_semaphore()
    for peer in (x_peers[2], x_peers[0], x_peers[1]):
        pl.semaphore_signal(barrier, inc=1, device_id=peer, device_id_type=MESH)

    def load(part, k):
        rows = pl.ds(LOADS[part], LOADS[part + 1] - LOADS[part])
        return pltpu.make_async_copy((w_hbm, a_hbm)[k].at[rows], buf.at[k, rows], load_sem.at[part])

    def wait_for(ref, sem):
        pltpu.make_async_copy(ref, ref, sem).wait()

    def loaded(part):
        wait_for(buf.at[:, pl.ds(LOADS[part], LOADS[part + 1] - LOADS[part])], load_sem.at[part])

    def remote(src, dst, send, recv, peer):
        return pltpu.make_async_remote_copy(
            src_ref=src, dst_ref=dst, send_sem=send, recv_sem=recv, device_id=peer, device_id_type=MESH
        )

    for part in range(len(LOADS) - 1):
        load(part, 0).start()
        load(part, 1).start()
        if part == 0:
            pltpu.make_async_copy(rw_hbm, small.at[0], small_sem).start()
            pltpu.make_async_copy(gain_hbm, small.at[1], small_sem).start()

    links = (
        (c == 1, c == 0, mate),
        (y < NY - 1, y == NY - 1, y_up),
        (y == 0, y > 0, y_down),
        *((z < NZ - hop, z >= NZ - hop, z_peer(hop)) for hop in (1, 3)),
        *((z < hop, z >= hop, z_peer(-hop)) for hop in (1, 3)),
    )
    entries, greetings = 3, 0
    for leads, follows, peer in links:
        entries += follows.astype(jnp.int32)
        greetings += leads.astype(jnp.int32)

        @pl.when(leads)
        def _(peer=peer):
            pl.semaphore_signal(barrier, inc=1, device_id=peer, device_id_type=MESH)

    def rows_of(b):
        return pl.ds(pl.multiple_of(b * BLK, BLK), BLK)

    def columns(start, width):
        return pl.ds(pl.multiple_of(start, 128), width)

    def average(b):
        here = rows_of(b)
        top = None
        for k in range(COLS // 128):
            lanes = pl.ds(k * 128, 128)
            value = 0.5 * buf[1, here, lanes] + 0.5 * buf[0, here, lanes]
            fresh[here, lanes] = value
            top = jnp.abs(value) if top is None else jnp.maximum(top, jnp.abs(value))
        return jnp.max(top.T, axis=0, keepdims=True)

    loaded(0)
    for b in range(2):
        m0[x, b : b + 1, :] = average(b)
    pl.semaphore_wait(barrier, entries)

    for k in (2, 0, 1):
        remote(m0.at[x], m0.at[x], m_send.at[0], m_recv.at[0], x_peers[k]).start()
    for d in range(2):
        remote(fresh.at[pl.ds(0, NE)], early.at[d], e_send, e_recv, x_peers[d]).start()
    wait_for(small, small_sem)
    part = small[0] * small[1]
    for k in range(NX):
        piece[lo, x, k : k + 1, :] = part[:, k * 128 : (k + 1) * 128]
    for k in range(3):
        remote(piece.at[lo, x], piece.at[lo, x], r0_send, r0_recv, x_peers[k]).start()
    for _, follows, peer in links:

        @pl.when(follows)
        def _(peer=peer):
            pl.semaphore_signal(greeted, inc=1, device_id=peer, device_id_type=MESH)

    def maxima(b, carry):
        m1[x, pl.ds(b - 2, 1), :] = average(b)
        return carry

    for part in range(1, len(LOADS) - 1):
        loaded(part)
        lax.fori_loop(LOADS[part] // BLK, LOADS[part + 1] // BLK, maxima, 0)
    for k in (2, 0, 1):
        remote(m1.at[x], m1.at[x], m_send.at[1], m_recv.at[1], x_peers[k]).start()

    mine = x * COLS

    def tall(top):
        return jnp.broadcast_to(top, (BLK, BLK)).T

    def narrow(src, here, start, scales):
        for k in range(COLS // 128):
            value = src[here, pl.ds(k * 128, 128)] / scales
            serve[here, columns(start + k * 128, 128)] = value.astype(BF16)

    def own(rows, h, d):
        ref = serve.at[rows, columns(mine + h * HALF, HALF)]
        return remote(ref, ref, own_send, pass_recv.at[d] if h == d else keep_recv, x_peers[d])

    def forward(n, d):
        ref = serve.at[pl.ds(0, n), columns((left if d == 0 else right) * COLS + d * HALF, HALF)]
        return remote(ref, ref, fwd_send, fwd_recv, x_peers[d])

    def by_core(do):
        for core, n in enumerate(RS):
            pl.when(c == core)(lambda n=n: do(n))

    chip = piece.at[pl.ds(y * NC, NC)]
    below = piece.at[pl.ds(lax.rem(y + NY - 1, NY) * NC, NC)]

    def send_plane(hop, k, step):
        plane = router.at[lax.rem(z + NZ + k, NZ)]
        remote(plane, plane, r3_send, r3_recv.at[step], z_peer(hop)).start()

    wait_for(m0.at[pl.ds(0, 3)], m_recv.at[0])
    top = jnp.maximum(jnp.maximum(m0[0], m0[1]), jnp.maximum(m0[2], m0[3]))
    scale[:, 0:BLK] = top[0:1]
    scale[:, BLK : 2 * BLK] = top[1:2]
    scales = tall(top[0:1])
    narrow(fresh, pl.ds(NE, BLK - NE), mine, scales[NE:])
    narrow(fresh, rows_of(1), mine, tall(top[1:2]))
    for h, d in ((0, 0), (1, 1), (1, 0), (0, 1)):
        own(pl.ds(NE, 2 * BLK - NE), h, d).start()
    narrow(fresh, pl.ds(0, NE), mine, scales[:NE])

    wait_for(m1.at[pl.ds(0, 3)], m_recv.at[1])

    def narrowed(b, carry):
        at = pl.ds(b - 2, 1)
        top = jnp.maximum(jnp.maximum(m1[0, at], m1[1, at]), jnp.maximum(m1[2, at], m1[3, at]))
        scale[:, columns(b * BLK, BLK)] = top
        narrow(fresh, rows_of(b), mine, tall(top))
        return carry

    lax.fori_loop(2, NB, narrowed, 0)

    @by_core
    def _(n):
        for h, d in ((0, 0), (1, 1), (1, 0), (0, 1)):
            own(pl.ds(2 * BLK, n - 2 * BLK), h, d).start()

    wait_for(early, e_recv)
    scales = tall(scale[:, 0:BLK])
    for d, peer in ((0, left), (1, right)):
        narrow(early.at[d], pl.ds(0, NE), peer * COLS, scales[:NE])

    @pl.when(greetings > 0)
    def _():
        pl.semaphore_wait(greeted, greetings)

    wait_for(piece.at[lo, pl.ds(0, 3)], r0_recv)
    remote(piece.at[lo], piece.at[lo], r12_send, r1_recv, mate).start()
    wait_for(piece.at[0], r1_recv)
    remote(chip, chip, r12_send, r2_recv.at[0], y_up).start()
    remote(chip, chip, r12_send, r2_recv.at[1], y_down).start()
    wait_for(chip, r2_recv.at[0])
    remote(below, below, r12_send, r2_recv.at[1], y_up).start()
    wait_for(piece.at[pl.ds(0, 2 * NC)], r2_recv.at[1])
    for i in range(NY * NC):
        for k in range(WIDE // 128):
            wide[i : i + 1, k * 128 : (k + 1) * 128] = piece[i, k // 4, k % 4 : k % 4 + 1, :]
    router[z] = wide[...].astype(BF16)
    send_plane(1, 0, 0)
    send_plane(-1, 0, 0)

    @by_core
    def _(n):
        for d in range(2):
            wait_for(serve.at[pl.ds(NE, n - NE), columns(0, HALF)], pass_recv.at[d])
            forward(n, d).start()

    wait_for(router.at[pl.ds(0, 2)], r3_recv.at[0])
    for k in (0, 1):
        send_plane(3, k, 1)
    for k in (-1, 0, 1):
        send_plane(-3, k, 1)
    wait_for(router.at[pl.ds(0, 5)], r3_recv.at[1])

    wait_for(early, e_send)
    for k, m in enumerate((m0, m1)):
        wait_for(m.at[pl.ds(0, 3)], m_send.at[k])
    wait_for(piece.at[0, pl.ds(0, 3)], r0_send)
    wait_for(piece.at[pl.ds(0, 1 + 3 * NC)], r12_send)
    wait_for(router.at[pl.ds(0, NZ - 1)], r3_send)

    @by_core
    def _(n):
        wait_for(serve.at[pl.ds(NE, n - NE), columns(0, COLS)], keep_recv)
        wait_for(serve.at[pl.ds(NE, n - NE), columns(0, 2 * COLS)], own_send)
        wait_for(serve.at[pl.ds(0, n), columns(0, COLS)], fwd_send)
        wait_for(serve.at[pl.ds(0, n), columns(0, COLS)], fwd_recv)


def rest_kernel(serve, stored, rest, own_send, keep_recv, pass_recv, fwd_send, fwd_recv):
    x, c = lax.axis_index("fsdp"), lax.rem(lax.axis_index("ep"), NC)
    right, left = lax.rem(x + 1, NX), lax.rem(x + 3, NX)
    peers = ({"fsdp": right}, {"fsdp": left})
    barrier = pltpu.get_barrier_semaphore()
    for peer in peers:
        pl.semaphore_signal(barrier, inc=1, device_id=peer, device_id_type=MESH)
    pl.semaphore_wait(barrier, 2)

    def columns(start, width):
        return pl.ds(pl.multiple_of(start, 128), width)

    def wait_for(n, width, sem):
        ref = rest.at[pl.ds(0, n), columns(0, width)]
        pltpu.make_async_copy(ref, ref, sem).wait()

    def remote(src, dst, send, recv, d):
        return pltpu.make_async_remote_copy(
            src_ref=src, dst_ref=dst, send_sem=send, recv_sem=recv, device_id=peers[d], device_id_type=MESH
        )

    def gather_rest(first):
        n = ROWS - first
        for h, d in ((0, 0), (1, 1), (1, 0), (0, 1)):
            lanes = columns(x * COLS + h * HALF, HALF)
            src, dst = serve.at[pl.ds(first, n), lanes], rest.at[pl.ds(0, n), lanes]
            remote(src, dst, own_send, pass_recv.at[d] if h == d else keep_recv, d).start()
        for d, source in ((0, left), (1, right)):
            wait_for(n, HALF, pass_recv.at[d])
            ref = rest.at[pl.ds(0, n), columns(source * COLS + d * HALF, HALF)]
            remote(ref, ref, fwd_send, fwd_recv, d).start()
        wait_for(n, 2 * HALF, keep_recv)
        wait_for(n, 4 * HALF, own_send)
        wait_for(n, 2 * HALF, fwd_send)
        wait_for(n, 2 * HALF, fwd_recv)

    for core, first in enumerate(RS):
        pl.when(c == core)(lambda first=first: gather_rest(first))


def gather(w_down, avg_down, rw, gain):
    dma, any_, vmem = pltpu.SemaphoreType.DMA, pl.BlockSpec(memory_space=pl.ANY), pl.BlockSpec(memory_space=pltpu.VMEM)
    return pl.pallas_call(
        gather_kernel,
        out_shape=(
            pltpu.VMEM((ROWS, WIDE), BF16),
            pltpu.VMEM((ROWS, COLS), F32),
            pltpu.VMEM((1, ROWS), F32),
            pltpu.VMEM((NZ, NY * NC, WIDE), BF16),
        ),
        in_specs=[any_] * 4,
        out_specs=(vmem, vmem, vmem, vmem),
        scratch_shapes=[
            pltpu.VMEM((2, ROWS, COLS), F32),
            pltpu.VMEM((2, 1, COLS), F32),
            pltpu.VMEM((NX, 2, BLK), F32),
            pltpu.VMEM((NX, NB - 2, BLK), F32),
            pltpu.VMEM((2, NE, COLS), F32),
            pltpu.VMEM((NY * NC, NX, NX, 128), F32),
            pltpu.VMEM((NY * NC, WIDE), F32),
            dma((len(LOADS) - 1,)),
            dma,
            dma((2,)),
            dma((2,)),
            dma,
            dma,
            dma,
            dma,
            dma((2,)),
            dma,
            dma,
            dma,
            dma,
            dma,
            dma,
            dma((2,)),
            dma,
            dma((2,)),
            pltpu.SemaphoreType.REGULAR,
        ],
        compiler_params=pltpu.CompilerParams(
            collective_id=0, has_side_effects=True, vmem_limit_bytes=24 << 20
        ),
        name="gather",
    )(*(pltpu.with_memory_space_constraint(v, pltpu.HBM) for v in (w_down, avg_down, rw, gain)))


def gather_rest(serve, stored):
    dma, any_, vmem = pltpu.SemaphoreType.DMA, pl.BlockSpec(memory_space=pl.ANY), pl.BlockSpec(memory_space=pltpu.VMEM)
    return pl.pallas_call(
        rest_kernel,
        out_shape=pltpu.VMEM((REST, WIDE), BF16),
        in_specs=[vmem, any_],
        out_specs=vmem,
        scratch_shapes=[dma, dma, dma((2,)), dma, dma],
        compiler_params=pltpu.CompilerParams(
            collective_id=1, has_side_effects=True, vmem_limit_bytes=8 << 20
        ),
        name="gather_rest",
    )(pltpu.with_memory_space_constraint(serve, pltpu.VMEM), pltpu.with_memory_space_constraint(stored, pltpu.HBM))


def store_kernel(serve, fresh, scale, router, serve_out, fresh_out, scale_out, router_out, stored, sem):
    x, c = lax.axis_index("fsdp"), lax.rem(lax.axis_index("ep"), NC)
    mine = pl.ds(pl.multiple_of(x * COLS, COLS), COLS)

    def store_first(n):
        left = pl.ds(n, ROWS - n)
        copies = [
            pltpu.make_async_copy(fresh, fresh_out, sem.at[0]),
            pltpu.make_async_copy(scale, scale_out, sem.at[1]),
            pltpu.make_async_copy(router, router_out, sem.at[2]),
            pltpu.make_async_copy(serve.at[pl.ds(0, n)], serve_out.at[pl.ds(0, n)], sem.at[3]),
            pltpu.make_async_copy(serve.at[left, mine], serve_out.at[left, mine], sem.at[4]),
        ]
        for copy in copies:
            copy.start()
        for copy in copies:
            copy.wait()

    for core, n in enumerate(RS):
        pl.when(c == core)(lambda n=n: store_first(n))


def store(serve, fresh, scale, router):
    vmem, any_ = pl.BlockSpec(memory_space=pltpu.VMEM), pl.BlockSpec(memory_space=pl.ANY)
    return pl.pallas_call(
        store_kernel,
        out_shape=(*(pltpu.HBM(v.shape, v.dtype) for v in (serve, fresh, scale, router)), pltpu.HBM((8, 128), F32)),
        in_specs=[vmem] * 4,
        out_specs=(any_,) * 5,
        scratch_shapes=[pltpu.SemaphoreType.DMA((5,))],
        compiler_params=pltpu.CompilerParams(vmem_limit_bytes=16 << 20),
        name="store",
    )(*(pltpu.with_memory_space_constraint(v, pltpu.VMEM) for v in (serve, fresh, scale, router)))


def store_rest_kernel(rest, serve_in, serve_out, sem):
    x, c = lax.axis_index("fsdp"), lax.rem(lax.axis_index("ep"), NC)

    def store_last(first):
        n = ROWS - first
        copies = []
        for k in range(1, NX):
            lanes = pl.ds(pl.multiple_of(lax.rem(x + k, NX) * COLS, COLS), COLS)
            src, dst = rest.at[pl.ds(0, n), lanes], serve_out.at[pl.ds(first, n), lanes]
            copies.append(pltpu.make_async_copy(src, dst, sem.at[k - 1]))
        for copy in copies:
            copy.start()
        for copy in copies:
            copy.wait()

    for core, first in enumerate(RS):
        pl.when(c == core)(lambda first=first: store_last(first))


def store_rest(rest, serve):
    vmem, any_ = pl.BlockSpec(memory_space=pltpu.VMEM), pl.BlockSpec(memory_space=pl.ANY)
    return pl.pallas_call(
        store_rest_kernel,
        out_shape=pltpu.HBM(serve.shape, serve.dtype),
        in_specs=[vmem, any_],
        out_specs=any_,
        input_output_aliases={1: 0},
        scratch_shapes=[pltpu.SemaphoreType.DMA((NX - 1,))],
        compiler_params=pltpu.CompilerParams(vmem_limit_bytes=8 << 20),
        name="store_rest",
    )(pltpu.with_memory_space_constraint(rest, pltpu.VMEM), pltpu.with_memory_space_constraint(serve, pltpu.HBM))


def body(w_down, avg_down, router_weight, router_gain):
    gathered, fresh, scale, router = gather(
        w_down.reshape(ROWS, COLS),
        avg_down.reshape(ROWS, COLS),
        router_weight.reshape(1, COLS),
        router_gain.reshape(1, COLS),
    )
    serve, fresh, scale, router, stored = store(gathered, fresh, scale, router)
    serve = store_rest(gather_rest(gathered, stored), serve)
    return (
        serve.reshape(1, ROWS, WIDE),
        scale,
        router.reshape(NZ * NY * NC, WIDE).T,
        fresh.reshape(1, ROWS, COLS),
    )


def solution(mesh):
    placed = (P("ep", None, "fsdp"), P("ep", None, "fsdp"), P("fsdp", "ep"), P("fsdp"))
    return jax.shard_map(
        body,
        mesh=mesh,
        in_specs=placed,
        out_specs=(P("ep", None, None), P("ep", None), P(), P("ep", None, "fsdp")),
        check_vma=False,
    )
```

```python
import jax
import jax.numpy as jnp
from jax import lax
from jax.experimental import pallas as pl
from jax.experimental.pallas import tpu as pltpu
from jax.sharding import PartitionSpec as P

MESH = pl.DeviceIdType.MESH
F32, BF16 = jnp.float32, jnp.bfloat16
NX, NY, NZ, NC = 4, 4, 8, 2
ROWS, COLS = 1408, 512
WIDE = NX * COLS
HALF = COLS // 2
BLK = 128
NB = ROWS // BLK
NE = 48


PASS = (ROWS, 736)
KEEP = (672, 736)
REST = ROWS - min(KEEP)
LOADS = (0, 256, 768, 1408)


def gather_kernel(
    w_hbm, a_hbm, rw_hbm, gain_hbm, serve, fresh, scale, router,
    buf, small, m0, m1, early, piece, wide,
    load_sem, small_sem, m_send, m_recv, e_send, e_recv, own_send, keep_recv, pass_recv, fwd_send, fwd_recv,
    r0_send, r0_recv, r12_send, r1_recv, r2_recv, r3_send, r3_recv, greeted,
):
    x, e = lax.axis_index("fsdp"), lax.axis_index("ep")
    right, far, left = lax.rem(x + 1, NX), lax.rem(x + 2, NX), lax.rem(x + 3, NX)
    lo = lax.rem(e, NY * NC)
    z, y, c = e // (NY * NC), lo // NC, lax.rem(lo, NC)
    x_peers = ({"fsdp": right}, {"fsdp": left}, {"fsdp": far})
    mate = {"ep": e + 1 - 2 * c}
    y_up = {"ep": z * (NY * NC) + lax.rem(y + 1, NY) * NC + c}
    y_down = {"ep": z * (NY * NC) + lax.rem(y + NY - 1, NY) * NC + c}

    def z_peer(hop):
        return {"ep": lax.rem(z + NZ + hop, NZ) * (NY * NC) + lo}


    barrier = pltpu.get_barrier_semaphore()
    for peer in (x_peers[2], x_peers[0], x_peers[1]):
        pl.semaphore_signal(barrier, inc=1, device_id=peer, device_id_type=MESH)

    def load(part, k):
        rows = pl.ds(LOADS[part], LOADS[part + 1] - LOADS[part])
        return pltpu.make_async_copy((w_hbm, a_hbm)[k].at[rows], buf.at[k, rows], load_sem.at[part])

    def wait_for(ref, sem):
        pltpu.make_async_copy(ref, ref, sem).wait()

    def loaded(part):
        wait_for(buf.at[:, pl.ds(LOADS[part], LOADS[part + 1] - LOADS[part])], load_sem.at[part])

    def remote(src, dst, send, recv, peer):
        return pltpu.make_async_remote_copy(
            src_ref=src, dst_ref=dst, send_sem=send, recv_sem=recv, device_id=peer, device_id_type=MESH
        )

    for part in range(len(LOADS) - 1):
        load(part, 0).start()
        load(part, 1).start()
        if part == 0:
            pltpu.make_async_copy(rw_hbm, small.at[0], small_sem).start()
            pltpu.make_async_copy(gain_hbm, small.at[1], small_sem).start()

    links = (
        (c == 1, c == 0, mate),
        (y < NY - 1, y == NY - 1, y_up),
        (y == 0, y > 0, y_down),
        *((z < NZ - hop, z >= NZ - hop, z_peer(hop)) for hop in (1, 3)),
        *((z < hop, z >= hop, z_peer(-hop)) for hop in (1, 3)),
    )
    entries, greetings = 3, 0
    for leads, follows, peer in links:
        entries += follows.astype(jnp.int32)
        greetings += leads.astype(jnp.int32)

        @pl.when(leads)
        def _(peer=peer):
            pl.semaphore_signal(barrier, inc=1, device_id=peer, device_id_type=MESH)

    def rows_of(b):
        return pl.ds(pl.multiple_of(b * BLK, BLK), BLK)

    def columns(start, width):
        return pl.ds(pl.multiple_of(start, 128), width)

    def average(b):
        here = rows_of(b)
        top = None
        for k in range(COLS // 128):
            lanes = pl.ds(k * 128, 128)
            value = 0.5 * buf[1, here, lanes] + 0.5 * buf[0, here, lanes]
            fresh[here, lanes] = value
            top = jnp.abs(value) if top is None else jnp.maximum(top, jnp.abs(value))
        return jnp.max(top.T, axis=0, keepdims=True)

    loaded(0)
    for b in range(2):
        m0[x, b : b + 1, :] = average(b)
    pl.semaphore_wait(barrier, entries)

    for k in (2, 0, 1):
        remote(m0.at[x], m0.at[x], m_send.at[0], m_recv.at[0], x_peers[k]).start()
    for d in range(2):
        remote(fresh.at[pl.ds(0, NE)], early.at[d], e_send, e_recv, x_peers[d]).start()
    wait_for(small, small_sem)
    part = small[0] * small[1]
    for k in range(NX):
        piece[lo, x, k : k + 1, :] = part[:, k * 128 : (k + 1) * 128]
    for k in range(3):
        remote(piece.at[lo, x], piece.at[lo, x], r0_send, r0_recv, x_peers[k]).start()
    for _, follows, peer in links:

        @pl.when(follows)
        def _(peer=peer):
            pl.semaphore_signal(greeted, inc=1, device_id=peer, device_id_type=MESH)

    def maxima(b, carry):
        m1[x, pl.ds(b - 2, 1), :] = average(b)
        return carry

    for part in range(1, len(LOADS) - 1):
        loaded(part)
        lax.fori_loop(LOADS[part] // BLK, LOADS[part + 1] // BLK, maxima, 0)
    for k in (2, 0, 1):
        remote(m1.at[x], m1.at[x], m_send.at[1], m_recv.at[1], x_peers[k]).start()

    mine = x * COLS

    def tall(top):
        return jnp.broadcast_to(top, (BLK, BLK)).T

    def narrow(src, here, start, scales):
        for k in range(COLS // 128):
            value = src[here, pl.ds(k * 128, 128)] / scales
            serve[here, columns(start + k * 128, 128)] = value.astype(BF16)

    def own(rows, h, d):
        ref = serve.at[rows, columns(mine + h * HALF, HALF)]
        return remote(ref, ref, own_send, pass_recv.at[d] if h == d else keep_recv, x_peers[d])

    def forward(n, d):
        ref = serve.at[pl.ds(0, n), columns((left if d == 0 else right) * COLS + d * HALF, HALF)]
        return remote(ref, ref, fwd_send, fwd_recv, x_peers[d])

    def by_core(do):
        for core in range(NC):
            pl.when(c == core)(lambda core=core: do(PASS[core], KEEP[core]))

    chip = piece.at[pl.ds(y * NC, NC)]
    below = piece.at[pl.ds(lax.rem(y + NY - 1, NY) * NC, NC)]

    def send_plane(hop, k, step):
        plane = router.at[lax.rem(z + NZ + k, NZ)]
        remote(plane, plane, r3_send, r3_recv.at[step], z_peer(hop)).start()

    wait_for(m0.at[pl.ds(0, 3)], m_recv.at[0])
    top = jnp.maximum(jnp.maximum(m0[0], m0[1]), jnp.maximum(m0[2], m0[3]))
    scale[:, 0:BLK] = top[0:1]
    scale[:, BLK : 2 * BLK] = top[1:2]
    scales = tall(top[0:1])
    narrow(fresh, pl.ds(NE, BLK - NE), mine, scales[NE:])
    narrow(fresh, rows_of(1), mine, tall(top[1:2]))
    for h, d in ((0, 0), (1, 1), (1, 0), (0, 1)):
        own(pl.ds(NE, 2 * BLK - NE), h, d).start()
    narrow(fresh, pl.ds(0, NE), mine, scales[:NE])

    wait_for(m1.at[pl.ds(0, 3)], m_recv.at[1])

    def narrowed(b, carry):
        at = pl.ds(b - 2, 1)
        top = jnp.maximum(jnp.maximum(m1[0, at], m1[1, at]), jnp.maximum(m1[2, at], m1[3, at]))
        scale[:, columns(b * BLK, BLK)] = top
        narrow(fresh, rows_of(b), mine, tall(top))
        return carry

    lax.fori_loop(2, NB, narrowed, 0)

    @by_core
    def _(passed, kept):
        for n, h, d in ((passed, 0, 0), (passed, 1, 1), (kept, 1, 0), (kept, 0, 1)):
            own(pl.ds(2 * BLK, n - 2 * BLK), h, d).start()

    wait_for(early, e_recv)
    scales = tall(scale[:, 0:BLK])
    for d, peer in ((0, left), (1, right)):
        narrow(early.at[d], pl.ds(0, NE), peer * COLS, scales[:NE])

    @pl.when(greetings > 0)
    def _():
        pl.semaphore_wait(greeted, greetings)

    wait_for(piece.at[lo, pl.ds(0, 3)], r0_recv)
    remote(piece.at[lo], piece.at[lo], r12_send, r1_recv, mate).start()
    wait_for(piece.at[0], r1_recv)
    remote(chip, chip, r12_send, r2_recv.at[0], y_up).start()
    remote(chip, chip, r12_send, r2_recv.at[1], y_down).start()
    wait_for(chip, r2_recv.at[0])
    remote(below, below, r12_send, r2_recv.at[1], y_up).start()
    wait_for(piece.at[pl.ds(0, 2 * NC)], r2_recv.at[1])
    for i in range(NY * NC):
        for k in range(WIDE // 128):
            wide[i : i + 1, k * 128 : (k + 1) * 128] = piece[i, k // 4, k % 4 : k % 4 + 1, :]
    router[z] = wide[...].astype(BF16)
    send_plane(1, 0, 0)
    send_plane(-1, 0, 0)

    @by_core
    def _(passed, kept):
        for d in range(2):
            wait_for(serve.at[pl.ds(NE, passed - NE), columns(0, HALF)], pass_recv.at[d])
            forward(passed, d).start()

    wait_for(router.at[pl.ds(0, 2)], r3_recv.at[0])
    for k in (0, 1):
        send_plane(3, k, 1)
    for k in (-1, 0, 1):
        send_plane(-3, k, 1)
    wait_for(router.at[pl.ds(0, 5)], r3_recv.at[1])

    wait_for(early, e_send)
    for k, m in enumerate((m0, m1)):
        wait_for(m.at[pl.ds(0, 3)], m_send.at[k])
    wait_for(piece.at[0, pl.ds(0, 3)], r0_send)
    wait_for(piece.at[pl.ds(0, 1 + 3 * NC)], r12_send)
    wait_for(router.at[pl.ds(0, NZ - 1)], r3_send)

    @by_core
    def _(passed, kept):
        wait_for(serve.at[pl.ds(NE, kept - NE), columns(0, COLS)], keep_recv)
        wait_for(serve.at[pl.ds(0, (passed + kept) // 2 - NE), columns(0, 2 * COLS)], own_send)
        wait_for(serve.at[pl.ds(0, passed), columns(0, COLS)], fwd_send)
        wait_for(serve.at[pl.ds(0, passed), columns(0, COLS)], fwd_recv)


def rest_kernel(serve, stored, rest, own_send, keep_recv, pass_recv, fwd_send, fwd_recv):
    x, c = lax.axis_index("fsdp"), lax.rem(lax.axis_index("ep"), NC)
    right, left = lax.rem(x + 1, NX), lax.rem(x + 3, NX)
    peers = ({"fsdp": right}, {"fsdp": left})
    barrier = pltpu.get_barrier_semaphore()
    for peer in peers:
        pl.semaphore_signal(barrier, inc=1, device_id=peer, device_id_type=MESH)
    pl.semaphore_wait(barrier, 2)

    def columns(start, width):
        return pl.ds(pl.multiple_of(start, 128), width)

    def wait_for(n, width, sem):
        ref = rest.at[pl.ds(0, n), columns(0, width)]
        pltpu.make_async_copy(ref, ref, sem).wait()

    def remote(src, dst, send, recv, d):
        return pltpu.make_async_remote_copy(
            src_ref=src, dst_ref=dst, send_sem=send, recv_sem=recv, device_id=peers[d], device_id_type=MESH
        )

    def gather_rest(first, with_far):
        n = ROWS - first
        for h, d in ((0, 0), (1, 1), (1, 0), (0, 1)):
            if h != d or with_far:
                lanes = columns(x * COLS + h * HALF, HALF)
                src, dst = serve.at[pl.ds(first, n), lanes], rest.at[pl.ds(0, n), lanes]
                remote(src, dst, own_send, pass_recv.at[d] if h == d else keep_recv, d).start()
        if with_far:
            for d, source in ((0, left), (1, right)):
                wait_for(n, HALF, pass_recv.at[d])
                ref = rest.at[pl.ds(0, n), columns(source * COLS + d * HALF, HALF)]
                remote(ref, ref, fwd_send, fwd_recv, d).start()
        wait_for(n, 2 * HALF, keep_recv)
        wait_for(n, (4 if with_far else 2) * HALF, own_send)
        if with_far:
            wait_for(n, 2 * HALF, fwd_send)
            wait_for(n, 2 * HALF, fwd_recv)

    for core in range(NC):
        pl.when(c == core)(lambda core=core: gather_rest(KEEP[core], PASS[core] < ROWS))


def gather(w_down, avg_down, rw, gain):
    dma, any_, vmem = pltpu.SemaphoreType.DMA, pl.BlockSpec(memory_space=pl.ANY), pl.BlockSpec(memory_space=pltpu.VMEM)
    return pl.pallas_call(
        gather_kernel,
        out_shape=(
            pltpu.VMEM((ROWS, WIDE), BF16),
            pltpu.VMEM((ROWS, COLS), F32),
            pltpu.VMEM((1, ROWS), F32),
            pltpu.VMEM((NZ, NY * NC, WIDE), BF16),
        ),
        in_specs=[any_] * 4,
        out_specs=(vmem, vmem, vmem, vmem),
        scratch_shapes=[
            pltpu.VMEM((2, ROWS, COLS), F32),
            pltpu.VMEM((2, 1, COLS), F32),
            pltpu.VMEM((NX, 2, BLK), F32),
            pltpu.VMEM((NX, NB - 2, BLK), F32),
            pltpu.VMEM((2, NE, COLS), F32),
            pltpu.VMEM((NY * NC, NX, NX, 128), F32),
            pltpu.VMEM((NY * NC, WIDE), F32),
            dma((len(LOADS) - 1,)),
            dma,
            dma((2,)),
            dma((2,)),
            dma,
            dma,
            dma,
            dma,
            dma((2,)),
            dma,
            dma,
            dma,
            dma,
            dma,
            dma,
            dma((2,)),
            dma,
            dma((2,)),
            pltpu.SemaphoreType.REGULAR,
        ],
        compiler_params=pltpu.CompilerParams(
            collective_id=0, has_side_effects=True, vmem_limit_bytes=24 << 20
        ),
        name="gather",
    )(*(pltpu.with_memory_space_constraint(v, pltpu.HBM) for v in (w_down, avg_down, rw, gain)))


def gather_rest(serve, stored):
    dma, any_, vmem = pltpu.SemaphoreType.DMA, pl.BlockSpec(memory_space=pl.ANY), pl.BlockSpec(memory_space=pltpu.VMEM)
    return pl.pallas_call(
        rest_kernel,
        out_shape=pltpu.VMEM((REST, WIDE), BF16),
        in_specs=[vmem, any_],
        out_specs=vmem,
        scratch_shapes=[dma, dma, dma((2,)), dma, dma],
        compiler_params=pltpu.CompilerParams(
            collective_id=1, has_side_effects=True, vmem_limit_bytes=8 << 20
        ),
        name="gather_rest",
    )(pltpu.with_memory_space_constraint(serve, pltpu.VMEM), pltpu.with_memory_space_constraint(stored, pltpu.HBM))


def store_kernel(serve, fresh, scale, router, serve_out, fresh_out, scale_out, router_out, stored, sem):
    x, c = lax.axis_index("fsdp"), lax.rem(lax.axis_index("ep"), NC)

    def columns(hop, half, width):
        return pl.ds(pl.multiple_of(lax.rem(x + hop, NX) * COLS + half * HALF, HALF), width)

    def store_first(passed, kept):
        pairs = [(fresh, fresh_out), (scale, scale_out), (router, router_out)]
        pieces = [(pl.ds(0, kept), pl.ds(0, WIDE)), (pl.ds(kept, ROWS - kept), columns(0, 0, COLS))]
        if kept < passed:
            arrived = pl.ds(kept, passed - kept)
            pieces += [(arrived, columns(2, 0, COLS)), (arrived, columns(3, 0, HALF)), (arrived, columns(1, 1, HALF))]
        pairs += [(serve.at[piece], serve_out.at[piece]) for piece in pieces]
        copies = [pltpu.make_async_copy(src, dst, sem.at[k]) for k, (src, dst) in enumerate(pairs)]
        for copy in copies:
            copy.start()
        for copy in copies:
            copy.wait()

    for core in range(NC):
        pl.when(c == core)(lambda core=core: store_first(PASS[core], KEEP[core]))


def store(serve, fresh, scale, router):
    vmem, any_ = pl.BlockSpec(memory_space=pltpu.VMEM), pl.BlockSpec(memory_space=pl.ANY)
    return pl.pallas_call(
        store_kernel,
        out_shape=(*(pltpu.HBM(v.shape, v.dtype) for v in (serve, fresh, scale, router)), pltpu.HBM((8, 128), F32)),
        in_specs=[vmem] * 4,
        out_specs=(any_,) * 5,
        scratch_shapes=[pltpu.SemaphoreType.DMA((8,))],
        compiler_params=pltpu.CompilerParams(vmem_limit_bytes=16 << 20),
        name="store",
    )(*(pltpu.with_memory_space_constraint(v, pltpu.VMEM) for v in (serve, fresh, scale, router)))


def store_rest_kernel(rest, serve_in, serve_out, sem):
    x, c = lax.axis_index("fsdp"), lax.rem(lax.axis_index("ep"), NC)

    def columns(hop, half, width):
        return pl.ds(pl.multiple_of(lax.rem(x + hop, NX) * COLS + half * HALF, HALF), width)

    def store_last(first, with_far):
        n = ROWS - first
        if with_far:
            pieces = [columns(hop, 0, COLS) for hop in (1, 2, 3)]
        else:
            pieces = [columns(3, 1, HALF), columns(1, 0, HALF)]
        copies = [
            pltpu.make_async_copy(rest.at[pl.ds(0, n), lanes], serve_out.at[pl.ds(first, n), lanes], sem.at[k])
            for k, lanes in enumerate(pieces)
        ]
        for copy in copies:
            copy.start()
        for copy in copies:
            copy.wait()

    for core in range(NC):
        pl.when(c == core)(lambda core=core: store_last(KEEP[core], PASS[core] < ROWS))


def store_rest(rest, serve):
    vmem, any_ = pl.BlockSpec(memory_space=pltpu.VMEM), pl.BlockSpec(memory_space=pl.ANY)
    return pl.pallas_call(
        store_rest_kernel,
        out_shape=pltpu.HBM(serve.shape, serve.dtype),
        in_specs=[vmem, any_],
        out_specs=any_,
        input_output_aliases={1: 0},
        scratch_shapes=[pltpu.SemaphoreType.DMA((NX - 1,))],
        compiler_params=pltpu.CompilerParams(vmem_limit_bytes=8 << 20),
        name="store_rest",
    )(pltpu.with_memory_space_constraint(rest, pltpu.VMEM), pltpu.with_memory_space_constraint(serve, pltpu.HBM))


def body(w_down, avg_down, router_weight, router_gain):
    gathered, fresh, scale, router = gather(
        w_down.reshape(ROWS, COLS),
        avg_down.reshape(ROWS, COLS),
        router_weight.reshape(1, COLS),
        router_gain.reshape(1, COLS),
    )
    serve, fresh, scale, router, stored = store(gathered, fresh, scale, router)
    serve = store_rest(gather_rest(gathered, stored), serve)
    return (
        serve.reshape(1, ROWS, WIDE),
        scale,
        router.reshape(NZ * NY * NC, WIDE).T,
        fresh.reshape(1, ROWS, COLS),
    )


def solution(mesh):
    placed = (P("ep", None, "fsdp"), P("ep", None, "fsdp"), P("fsdp", "ep"), P("fsdp"))
    return jax.shard_map(
        body,
        mesh=mesh,
        in_specs=placed,
        out_specs=(P("ep", None, None), P("ep", None), P(), P("ep", None, "fsdp")),
        check_vma=False,
    )
```

```python
import jax
import jax.numpy as jnp
from jax import lax
from jax.experimental import pallas as pl
from jax.experimental.pallas import tpu as pltpu
from jax.sharding import PartitionSpec as P

MESH = pl.DeviceIdType.MESH
F32, BF16 = jnp.float32, jnp.bfloat16
NX, NY, NZ, NC = 4, 4, 8, 2
ROWS, COLS = 1408, 512
WIDE = NX * COLS
HALF = COLS // 2
BLK = 128
NB = ROWS // BLK
NE = 48


PASS = (ROWS, 800)
KEEP = (736, 800)
REST = ROWS - min(KEEP)
LOADS = (0, 256, 768, 1408)


def gather_kernel(
    w_hbm, a_hbm, rw_hbm, gain_hbm, serve, fresh, scale, router,
    buf, small, m0, m1, early, piece, wide,
    load_sem, small_sem, m_send, m_recv, e_send, e_recv, own_send, keep_recv, pass_recv, fwd_send, fwd_recv,
    r0_send, r0_recv, r12_send, r1_recv, r2_recv, r3_send, r3_recv, greeted,
):
    x, e = lax.axis_index("fsdp"), lax.axis_index("ep")
    right, far, left = lax.rem(x + 1, NX), lax.rem(x + 2, NX), lax.rem(x + 3, NX)
    lo = lax.rem(e, NY * NC)
    z, y, c = e // (NY * NC), lo // NC, lax.rem(lo, NC)
    x_peers = ({"fsdp": right}, {"fsdp": left}, {"fsdp": far})
    mate = {"ep": e + 1 - 2 * c}
    y_up = {"ep": z * (NY * NC) + lax.rem(y + 1, NY) * NC + c}
    y_down = {"ep": z * (NY * NC) + lax.rem(y + NY - 1, NY) * NC + c}

    def z_peer(hop):
        return {"ep": lax.rem(z + NZ + hop, NZ) * (NY * NC) + lo}


    barrier = pltpu.get_barrier_semaphore()
    for peer in (x_peers[2], x_peers[0], x_peers[1]):
        pl.semaphore_signal(barrier, inc=1, device_id=peer, device_id_type=MESH)

    def load(part, k):
        rows = pl.ds(LOADS[part], LOADS[part + 1] - LOADS[part])
        return pltpu.make_async_copy((w_hbm, a_hbm)[k].at[rows], buf.at[k, rows], load_sem.at[part])

    def wait_for(ref, sem):
        pltpu.make_async_copy(ref, ref, sem).wait()

    def loaded(part):
        wait_for(buf.at[:, pl.ds(LOADS[part], LOADS[part + 1] - LOADS[part])], load_sem.at[part])

    def remote(src, dst, send, recv, peer):
        return pltpu.make_async_remote_copy(
            src_ref=src, dst_ref=dst, send_sem=send, recv_sem=recv, device_id=peer, device_id_type=MESH
        )

    for part in range(len(LOADS) - 1):
        load(part, 0).start()
        load(part, 1).start()
        if part == 0:
            pltpu.make_async_copy(rw_hbm, small.at[0], small_sem).start()
            pltpu.make_async_copy(gain_hbm, small.at[1], small_sem).start()

    links = (
        (c == 1, c == 0, mate),
        (y < NY - 1, y == NY - 1, y_up),
        (y == 0, y > 0, y_down),
        *((z < NZ - hop, z >= NZ - hop, z_peer(hop)) for hop in (1, 3)),
        *((z < hop, z >= hop, z_peer(-hop)) for hop in (1, 3)),
    )
    entries, greetings = 3, 0
    for leads, follows, peer in links:
        entries += follows.astype(jnp.int32)
        greetings += leads.astype(jnp.int32)

        @pl.when(leads)
        def _(peer=peer):
            pl.semaphore_signal(barrier, inc=1, device_id=peer, device_id_type=MESH)

    def rows_of(b):
        return pl.ds(pl.multiple_of(b * BLK, BLK), BLK)

    def columns(start, width):
        return pl.ds(pl.multiple_of(start, 128), width)

    def average(b):
        here = rows_of(b)
        top = None
        for k in range(COLS // 128):
            lanes = pl.ds(k * 128, 128)
            value = 0.5 * buf[1, here, lanes] + 0.5 * buf[0, here, lanes]
            fresh[here, lanes] = value
            top = jnp.abs(value) if top is None else jnp.maximum(top, jnp.abs(value))
        return jnp.max(top.T, axis=0, keepdims=True)

    loaded(0)
    for b in range(2):
        m0[x, b : b + 1, :] = average(b)
    pl.semaphore_wait(barrier, entries)

    for k in (2, 0, 1):
        remote(m0.at[x], m0.at[x], m_send.at[0], m_recv.at[0], x_peers[k]).start()
    for d in range(2):
        remote(fresh.at[pl.ds(0, NE)], early.at[d], e_send, e_recv, x_peers[d]).start()
    wait_for(small, small_sem)
    part = small[0] * small[1]
    for k in range(NX):
        piece[lo, x, k : k + 1, :] = part[:, k * 128 : (k + 1) * 128]
    for k in range(3):
        remote(piece.at[lo, x], piece.at[lo, x], r0_send, r0_recv, x_peers[k]).start()
    for _, follows, peer in links:

        @pl.when(follows)
        def _(peer=peer):
            pl.semaphore_signal(greeted, inc=1, device_id=peer, device_id_type=MESH)

    def maxima(b, carry):
        m1[x, pl.ds(b - 2, 1), :] = average(b)
        return carry

    for part in range(1, len(LOADS) - 1):
        loaded(part)
        lax.fori_loop(LOADS[part] // BLK, LOADS[part + 1] // BLK, maxima, 0)
    for k in (2, 0, 1):
        remote(m1.at[x], m1.at[x], m_send.at[1], m_recv.at[1], x_peers[k]).start()

    mine = x * COLS

    def tall(top):
        return jnp.broadcast_to(top, (BLK, BLK)).T

    def narrow(src, here, start, scales):
        for k in range(COLS // 128):
            value = src[here, pl.ds(k * 128, 128)] / scales
            serve[here, columns(start + k * 128, 128)] = value.astype(BF16)

    def own(rows, h, d):
        ref = serve.at[rows, columns(mine + h * HALF, HALF)]
        return remote(ref, ref, own_send, pass_recv.at[d] if h == d else keep_recv, x_peers[d])

    def forward(n, d):
        ref = serve.at[pl.ds(0, n), columns((left if d == 0 else right) * COLS + d * HALF, HALF)]
        return remote(ref, ref, fwd_send, fwd_recv, x_peers[d])

    def by_core(do):
        for core in range(NC):
            pl.when(c == core)(lambda core=core: do(PASS[core], KEEP[core]))

    chip = piece.at[pl.ds(y * NC, NC)]
    below = piece.at[pl.ds(lax.rem(y + NY - 1, NY) * NC, NC)]

    def send_plane(hop, k, step):
        plane = router.at[lax.rem(z + NZ + k, NZ)]
        remote(plane, plane, r3_send, r3_recv.at[step], z_peer(hop)).start()

    wait_for(m0.at[pl.ds(0, 3)], m_recv.at[0])
    top = jnp.maximum(jnp.maximum(m0[0], m0[1]), jnp.maximum(m0[2], m0[3]))
    scale[:, 0:BLK] = top[0:1]
    scale[:, BLK : 2 * BLK] = top[1:2]
    scales = tall(top[0:1])
    narrow(fresh, pl.ds(NE, BLK - NE), mine, scales[NE:])
    narrow(fresh, rows_of(1), mine, tall(top[1:2]))
    for h, d in ((0, 0), (1, 1), (1, 0), (0, 1)):
        own(pl.ds(NE, 2 * BLK - NE), h, d).start()
    narrow(fresh, pl.ds(0, NE), mine, scales[:NE])

    wait_for(m1.at[pl.ds(0, 3)], m_recv.at[1])

    def narrowed(b, carry):
        at = pl.ds(b - 2, 1)
        top = jnp.maximum(jnp.maximum(m1[0, at], m1[1, at]), jnp.maximum(m1[2, at], m1[3, at]))
        scale[:, columns(b * BLK, BLK)] = top
        narrow(fresh, rows_of(b), mine, tall(top))
        return carry

    lax.fori_loop(2, NB, narrowed, 0)

    @by_core
    def _(passed, kept):
        for n, h, d in ((passed, 0, 0), (passed, 1, 1), (kept, 1, 0), (kept, 0, 1)):
            own(pl.ds(2 * BLK, n - 2 * BLK), h, d).start()

    wait_for(early, e_recv)
    scales = tall(scale[:, 0:BLK])
    for d, peer in ((0, left), (1, right)):
        narrow(early.at[d], pl.ds(0, NE), peer * COLS, scales[:NE])

    @pl.when(greetings > 0)
    def _():
        pl.semaphore_wait(greeted, greetings)

    wait_for(piece.at[lo, pl.ds(0, 3)], r0_recv)
    remote(piece.at[lo], piece.at[lo], r12_send, r1_recv, mate).start()
    wait_for(piece.at[0], r1_recv)
    remote(chip, chip, r12_send, r2_recv.at[0], y_up).start()
    remote(chip, chip, r12_send, r2_recv.at[1], y_down).start()
    wait_for(chip, r2_recv.at[0])
    remote(below, below, r12_send, r2_recv.at[1], y_up).start()
    wait_for(piece.at[pl.ds(0, 2 * NC)], r2_recv.at[1])
    for i in range(NY * NC):
        for k in range(WIDE // 128):
            wide[i : i + 1, k * 128 : (k + 1) * 128] = piece[i, k // 4, k % 4 : k % 4 + 1, :]
    router[z] = wide[...].astype(BF16)
    send_plane(1, 0, 0)
    send_plane(-1, 0, 0)

    @by_core
    def _(passed, kept):
        for d in range(2):
            wait_for(serve.at[pl.ds(NE, passed - NE), columns(0, HALF)], pass_recv.at[d])
            forward(passed, d).start()

    wait_for(router.at[pl.ds(0, 2)], r3_recv.at[0])
    for k in (0, 1):
        send_plane(3, k, 1)
    for k in (-1, 0, 1):
        send_plane(-3, k, 1)
    wait_for(router.at[pl.ds(0, 5)], r3_recv.at[1])

    wait_for(early, e_send)
    for k, m in enumerate((m0, m1)):
        wait_for(m.at[pl.ds(0, 3)], m_send.at[k])
    wait_for(piece.at[0, pl.ds(0, 3)], r0_send)
    wait_for(piece.at[pl.ds(0, 1 + 3 * NC)], r12_send)
    wait_for(router.at[pl.ds(0, NZ - 1)], r3_send)

    @by_core
    def _(passed, kept):
        wait_for(serve.at[pl.ds(NE, kept - NE), columns(0, COLS)], keep_recv)
        wait_for(serve.at[pl.ds(0, (passed + kept) // 2 - NE), columns(0, 2 * COLS)], own_send)
        wait_for(serve.at[pl.ds(0, passed), columns(0, COLS)], fwd_send)
        wait_for(serve.at[pl.ds(0, passed), columns(0, COLS)], fwd_recv)


def rest_kernel(serve, stored, rest, own_send, keep_recv, pass_recv, fwd_send, fwd_recv):
    x, c = lax.axis_index("fsdp"), lax.rem(lax.axis_index("ep"), NC)
    right, left = lax.rem(x + 1, NX), lax.rem(x + 3, NX)
    peers = ({"fsdp": right}, {"fsdp": left})
    barrier = pltpu.get_barrier_semaphore()
    for peer in peers:
        pl.semaphore_signal(barrier, inc=1, device_id=peer, device_id_type=MESH)
    pl.semaphore_wait(barrier, 2)

    def columns(start, width):
        return pl.ds(pl.multiple_of(start, 128), width)

    def wait_for(n, width, sem):
        ref = rest.at[pl.ds(0, n), columns(0, width)]
        pltpu.make_async_copy(ref, ref, sem).wait()

    def remote(src, dst, send, recv, d):
        return pltpu.make_async_remote_copy(
            src_ref=src, dst_ref=dst, send_sem=send, recv_sem=recv, device_id=peers[d], device_id_type=MESH
        )

    def gather_rest(first, with_far):
        n = ROWS - first
        for h, d in ((0, 0), (1, 1), (1, 0), (0, 1)):
            if h != d or with_far:
                lanes = columns(x * COLS + h * HALF, HALF)
                src, dst = serve.at[pl.ds(first, n), lanes], rest.at[pl.ds(0, n), lanes]
                remote(src, dst, own_send, pass_recv.at[d] if h == d else keep_recv, d).start()
        if with_far:
            for d, source in ((0, left), (1, right)):
                wait_for(n, HALF, pass_recv.at[d])
                ref = rest.at[pl.ds(0, n), columns(source * COLS + d * HALF, HALF)]
                remote(ref, ref, fwd_send, fwd_recv, d).start()
        wait_for(n, 2 * HALF, keep_recv)
        wait_for(n, (4 if with_far else 2) * HALF, own_send)
        if with_far:
            wait_for(n, 2 * HALF, fwd_send)
            wait_for(n, 2 * HALF, fwd_recv)

    for core in range(NC):
        pl.when(c == core)(lambda core=core: gather_rest(KEEP[core], PASS[core] < ROWS))


def gather(w_down, avg_down, rw, gain):
    dma, any_, vmem = pltpu.SemaphoreType.DMA, pl.BlockSpec(memory_space=pl.ANY), pl.BlockSpec(memory_space=pltpu.VMEM)
    return pl.pallas_call(
        gather_kernel,
        out_shape=(
            pltpu.VMEM((ROWS, WIDE), BF16),
            pltpu.VMEM((ROWS, COLS), F32),
            pltpu.VMEM((1, ROWS), F32),
            pltpu.VMEM((NZ, NY * NC, WIDE), BF16),
        ),
        in_specs=[any_] * 4,
        out_specs=(vmem, vmem, vmem, vmem),
        scratch_shapes=[
            pltpu.VMEM((2, ROWS, COLS), F32),
            pltpu.VMEM((2, 1, COLS), F32),
            pltpu.VMEM((NX, 2, BLK), F32),
            pltpu.VMEM((NX, NB - 2, BLK), F32),
            pltpu.VMEM((2, NE, COLS), F32),
            pltpu.VMEM((NY * NC, NX, NX, 128), F32),
            pltpu.VMEM((NY * NC, WIDE), F32),
            dma((len(LOADS) - 1,)),
            dma,
            dma((2,)),
            dma((2,)),
            dma,
            dma,
            dma,
            dma,
            dma((2,)),
            dma,
            dma,
            dma,
            dma,
            dma,
            dma,
            dma((2,)),
            dma,
            dma((2,)),
            pltpu.SemaphoreType.REGULAR,
        ],
        compiler_params=pltpu.CompilerParams(
            collective_id=0, has_side_effects=True, vmem_limit_bytes=24 << 20
        ),
        name="gather",
    )(*(pltpu.with_memory_space_constraint(v, pltpu.HBM) for v in (w_down, avg_down, rw, gain)))


def gather_rest(serve, stored):
    dma, any_, vmem = pltpu.SemaphoreType.DMA, pl.BlockSpec(memory_space=pl.ANY), pl.BlockSpec(memory_space=pltpu.VMEM)
    return pl.pallas_call(
        rest_kernel,
        out_shape=pltpu.VMEM((REST, WIDE), BF16),
        in_specs=[vmem, any_],
        out_specs=vmem,
        scratch_shapes=[dma, dma, dma((2,)), dma, dma],
        compiler_params=pltpu.CompilerParams(
            collective_id=1, has_side_effects=True, vmem_limit_bytes=8 << 20
        ),
        name="gather_rest",
    )(pltpu.with_memory_space_constraint(serve, pltpu.VMEM), pltpu.with_memory_space_constraint(stored, pltpu.HBM))


def store_kernel(serve, fresh, scale, router, serve_out, fresh_out, scale_out, router_out, stored, sem):
    x, c = lax.axis_index("fsdp"), lax.rem(lax.axis_index("ep"), NC)

    def columns(hop, half, width):
        return pl.ds(pl.multiple_of(lax.rem(x + hop, NX) * COLS + half * HALF, HALF), width)

    def store_first(passed, kept):
        pairs = [(fresh, fresh_out), (scale, scale_out), (router, router_out)]
        pieces = [(pl.ds(0, kept), pl.ds(0, WIDE)), (pl.ds(kept, ROWS - kept), columns(0, 0, COLS))]
        if kept < passed:
            arrived = pl.ds(kept, passed - kept)
            pieces += [(arrived, columns(2, 0, COLS)), (arrived, columns(3, 0, HALF)), (arrived, columns(1, 1, HALF))]
        pairs += [(serve.at[piece], serve_out.at[piece]) for piece in pieces]
        copies = [pltpu.make_async_copy(src, dst, sem.at[k]) for k, (src, dst) in enumerate(pairs)]
        for copy in copies:
            copy.start()
        for copy in copies:
            copy.wait()

    for core in range(NC):
        pl.when(c == core)(lambda core=core: store_first(PASS[core], KEEP[core]))


def store(serve, fresh, scale, router):
    vmem, any_ = pl.BlockSpec(memory_space=pltpu.VMEM), pl.BlockSpec(memory_space=pl.ANY)
    return pl.pallas_call(
        store_kernel,
        out_shape=(*(pltpu.HBM(v.shape, v.dtype) for v in (serve, fresh, scale, router)), pltpu.HBM((8, 128), F32)),
        in_specs=[vmem] * 4,
        out_specs=(any_,) * 5,
        scratch_shapes=[pltpu.SemaphoreType.DMA((8,))],
        compiler_params=pltpu.CompilerParams(vmem_limit_bytes=16 << 20),
        name="store",
    )(*(pltpu.with_memory_space_constraint(v, pltpu.VMEM) for v in (serve, fresh, scale, router)))


def store_rest_kernel(rest, serve_in, serve_out, sem):
    x, c = lax.axis_index("fsdp"), lax.rem(lax.axis_index("ep"), NC)

    def columns(hop, half, width):
        return pl.ds(pl.multiple_of(lax.rem(x + hop, NX) * COLS + half * HALF, HALF), width)

    def store_last(first, with_far):
        n = ROWS - first
        if with_far:
            pieces = [columns(hop, 0, COLS) for hop in (1, 2, 3)]
        else:
            pieces = [columns(3, 1, HALF), columns(1, 0, HALF)]
        half = n // 2
        parts = [(lanes, start) for lanes in pieces for start in (0, half)]
        copies = [
            pltpu.make_async_copy(
                rest.at[pl.ds(start, half), lanes], serve_out.at[pl.ds(first + start, half), lanes], sem.at[k]
            )
            for k, (lanes, start) in enumerate(parts)
        ]
        for copy in copies:
            copy.start()
        for copy in copies:
            copy.wait()

    for core in range(NC):
        pl.when(c == core)(lambda core=core: store_last(KEEP[core], PASS[core] < ROWS))


def store_rest(rest, serve):
    vmem, any_ = pl.BlockSpec(memory_space=pltpu.VMEM), pl.BlockSpec(memory_space=pl.ANY)
    return pl.pallas_call(
        store_rest_kernel,
        out_shape=pltpu.HBM(serve.shape, serve.dtype),
        in_specs=[vmem, any_],
        out_specs=any_,
        input_output_aliases={1: 0},
        scratch_shapes=[pltpu.SemaphoreType.DMA((2 * (NX - 1),))],
        compiler_params=pltpu.CompilerParams(vmem_limit_bytes=8 << 20),
        name="store_rest",
    )(pltpu.with_memory_space_constraint(rest, pltpu.VMEM), pltpu.with_memory_space_constraint(serve, pltpu.HBM))


def body(w_down, avg_down, router_weight, router_gain):
    gathered, fresh, scale, router = gather(
        w_down.reshape(ROWS, COLS),
        avg_down.reshape(ROWS, COLS),
        router_weight.reshape(1, COLS),
        router_gain.reshape(1, COLS),
    )
    serve, fresh, scale, router, stored = store(gathered, fresh, scale, router)
    serve = store_rest(gather_rest(gathered, stored), serve)
    return (
        serve.reshape(1, ROWS, WIDE),
        scale,
        router.reshape(NZ * NY * NC, WIDE).T,
        fresh.reshape(1, ROWS, COLS),
    )


def solution(mesh):
    placed = (P("ep", None, "fsdp"), P("ep", None, "fsdp"), P("fsdp", "ep"), P("fsdp"))
    return jax.shard_map(
        body,
        mesh=mesh,
        in_specs=placed,
        out_specs=(P("ep", None, None), P("ep", None), P(), P("ep", None, "fsdp")),
        check_vma=False,
    )
```
